128 devices in a mesh: samp: 4 (over y), band: 32 (over z, x, core).
Axes of the slice: x: 4, y: 4, z: 4, core: 2. Of those that a mesh axis runs over, the one named last changes fastest.
Arguments:
- tod: float32 [32, 16384], P('band', 'samp'), may hold values from -6 to 6
- cycle: int32 [32, 16384], P('band', 'samp'), may hold values from 0 to 3
- phi_cell: int32 [32, 16384], P('band', 'samp'), may hold values from 0 to 8191
- psi_bin: int32 [32, 16384], P('band', 'samp'), may hold values from 0 to 32
- offset: int32 [32, 16384], P('band', 'samp'), may hold values from 0 to 7
- counts: int32 [32, 4], P('band', 'samp'), may hold values from 1 to 4096, as said below
- kernel: float32 [8, 4], replicated, may hold values from 0.1 to 1
- wigner: float32 [32, 80, 33, 64, 128], P('band', 'samp'), may hold values from -0.015625 to 0.015625
- beam: float32 [64, 33], replicated, may hold values from -1 to 1
Outputs:
- sky: float32 [32, 80, 128], P('band', 'samp')
The draws below stay inside these ranges and needn't reach their ends.
Inputs may be any that keep to these rules, and one draw needn't show every extreme that they name: counts[b, s] samples of shard s in band b are live, those at the first positions of the shard; some shard is full.
All inputs are finite; a program needn't handle non-finite values.
Results may differ from the reference program's by a relative error of at most 0.0025.
Values sent between devices are 32-bit elements; how exact they have to be, the bound alone decides.
No kernel may reach another device: no remote copies, remote signals or barrier semaphores. Data moves between devices by JAX's collectives and lax.ppermute only.
A program may use at most 128 MiB of HBM per device.

```python
import jax
import jax.numpy as jnp
from jax import lax

PHI = 8192
K = 33
M = 2560
LB = 64
R_BAND = 4
S_DEV = 4096
RT = 128
N_SAMP = 4
N_BAND = 32


def draw_counts(key, part):
    key_a = jax.random.fold_in(key, 11)
    key_b = jax.random.fold_in(key, 12)
    key_c = jax.random.fold_in(key, 13)
    shifts = jax.random.randint(key_a, (N_BAND, N_SAMP), 0, 4)
    base = jnp.right_shift(jnp.full((N_BAND, N_SAMP), S_DEV, jnp.int32), shifts)
    jitter = jax.random.randint(key_b, (N_BAND, N_SAMP), 0, max(S_DEV // 16, 1))
    values = jnp.maximum(base - jitter, 1).reshape(-1)
    chosen = jax.random.randint(key_c, (), 0, N_BAND * N_SAMP)
    values = jnp.where(jnp.arange(N_BAND * N_SAMP) == chosen, S_DEV, values)
    return values.reshape(N_BAND, N_SAMP).astype(jnp.int32)


def plant(values, rng, least, top_value):
    index_at = [jax.random.randint(jax.random.fold_in(rng, axis), (), 0, length) for axis, length in enumerate(values.shape)]
    main_axis = values.shape.index(max(values.shape))
    next_to = index_at[:main_axis] + [(index_at[main_axis] + 1) % values.shape[main_axis]] + index_at[main_axis + 1:]
    return values.at[tuple(index_at)].set(least).at[tuple(next_to)].set(top_value)


def level_of(key, shape, shards, smallest, high):
    gain = 1.0
    for dim, shards_of in shards:
        draws = jax.random.uniform(jax.random.fold_in(jax.random.fold_in(key, 6), dim), (shards_of,), jnp.float32, smallest / len(shards), high / len(shards))
        gain = gain * jnp.repeat(jnp.exp(draws), shape[dim] // shards_of).reshape((-1,) + (1,) * (len(shape) - 1 - dim))
    return gain


def noise(own_key, shape, scale, limit, pieces=(), kind=jnp.bfloat16):
    loudness = level_of(own_key, shape, pieces, -0.22, 0.18) if pieces else 1.0
    entries = jax.random.normal(own_key, shape, jnp.float32) * scale * loudness
    return jnp.minimum(jnp.maximum(entries, -limit), limit).astype(kind)


def setup_inputs(seed: int = 0) -> dict:
    keys = jax.random.split(jax.random.key(seed), 10)
    tod = noise(keys[0], (N_BAND, N_SAMP * S_DEV), 1.0, 6.0, ((0, 32), (1, 4)), jnp.float32)
    cycle = plant(jax.random.randint(keys[1], (N_BAND, N_SAMP * S_DEV), 0, R_BAND), jax.random.fold_in(keys[1], 1), 0, R_BAND - 1).astype(jnp.int32)
    phi_cell = plant(jax.random.randint(keys[2], (N_BAND, N_SAMP * S_DEV), 0, PHI), jax.random.fold_in(keys[2], 1), 0, PHI - 1).astype(jnp.int32)
    psi_bin = plant(jax.random.randint(keys[3], (N_BAND, N_SAMP * S_DEV), 0, K), jax.random.fold_in(keys[3], 1), 0, K - 1).astype(jnp.int32)
    offset = plant(jax.random.randint(keys[4], (N_BAND, N_SAMP * S_DEV), 0, 8), jax.random.fold_in(keys[4], 1), 0, 7).astype(jnp.int32)
    counts = draw_counts(jax.random.fold_in(keys[9], 71), 0)
    kernel = jnp.clip(jax.random.uniform(keys[6], (8, 4), jnp.float32, 0.1, 1.0), 0.1, 1.0)
    wigner = noise(keys[7], (N_BAND, M // N_BAND, K, LB, RT), (1024 * RT) ** -0.5, 0.015625, ((0, 32), (1, 4)), jnp.float32)
    beam = noise(keys[8], (LB, K), K ** -0.5, 1.0, (), jnp.float32)
    return dict(tod=tod, cycle=cycle, phi_cell=phi_cell, psi_bin=psi_bin, offset=offset, counts=counts, kernel=kernel, wigner=wigner, beam=beam)


def reference(tod, cycle, phi_cell, psi_bin, offset, counts, kernel, wigner, beam):
    bands, total = tod.shape
    slots = jnp.arange(total, dtype=jnp.int32)
    shard_of = slots // S_DEV
    live = ((slots % S_DEV)[None, :] < counts[:, shard_of]).astype(jnp.float32)
    weights = kernel[offset]
    deposit = (tod[..., None] * weights * live[..., None]).astype(jnp.bfloat16)
    deposit = lax.optimization_barrier(deposit).astype(jnp.float32)
    rows = jnp.arange(bands, dtype=jnp.int32)[:, None] * R_BAND + cycle
    taps = jnp.arange(4, dtype=jnp.int32) - 1
    cols = (phi_cell[..., None] + taps) % PHI
    rows_b = jnp.broadcast_to(rows[..., None], cols.shape)
    psi_b = jnp.broadcast_to(psi_bin[..., None], cols.shape)
    cube = jnp.zeros((bands * R_BAND, K, PHI), jnp.float32)
    cube = cube.at[rows_b, psi_b, cols].add(deposit)
    spec = jnp.fft.rfft(cube, axis=2)[:, :, :M]
    spec = jnp.fft.fft(spec, axis=1)
    stacked = jnp.stack([jnp.real(spec), jnp.imag(spec)], axis=2)
    stacked = jnp.transpose(stacked, (3, 0, 1, 2)).astype(jnp.float32)
    table = wigner.reshape(M, K, LB, bands * R_BAND)

    def one_order(pair):
        table_m, spec_m = pair
        partial_value = jnp.einsum("klt,tkc->kcl", table_m, spec_m, precision=lax.Precision.HIGHEST)
        return jnp.einsum("lk,kcl->cl", beam, partial_value, precision=lax.Precision.HIGHEST)

    result = lax.map(one_order, (table, stacked))
    return result.reshape(bands, M // bands, 2 * LB)
```

```python
import math

import jax
import jax.numpy as jnp
import numpy as np
from jax import lax
from jax.experimental import pallas as pl
from jax.experimental.pallas import tpu as pltpu
from jax.sharding import PartitionSpec as P

PHI = 8192
K = 33
M = 2560
LB = 64
S_DEV = 4096
RT = 128
PER_DEV = 20
ROWS = 32
BLOCK = 4
CELL_ROWS = 560
TILES = 11
BF = jnp.bfloat16


def split_host(x):
    x = np.asarray(x, np.float32)
    hi = x.astype(BF)
    lo = (x - hi.astype(np.float32)).astype(BF)
    return np.stack([hi, lo])


def host_tables():
    a = np.arange(16)
    cl = np.arange(16)
    ang = 2 * np.pi * ((a[:, None] * cl[None, :]) % 16) / 16
    fc, fs = np.cos(ang), -np.sin(ang)
    f_main = np.concatenate([np.repeat(fc, 32, 1), np.repeat(fs, 32, 1)], 1)
    f_last = np.zeros((128, 256))
    f_last[:16, :16] = fc
    f_last[:16, 128:144] = fs
    b = np.arange(512)
    m2 = (5 * np.arange(32)[None, :] + np.arange(5)[:, None]).reshape(-1)
    ang = 2 * np.pi * ((m2[:, None] * b[None, :]) % 512) / 512
    w_phi = np.concatenate([np.cos(ang), np.sin(ang)], 0)
    lanes = np.concatenate([np.arange(512) // 32, np.where(np.arange(128) < 16, np.arange(128), 0)])
    ang = 2 * np.pi * (16 * np.arange(33)[:, None] * lanes[None, :]) / PHI
    t_hi = np.stack([np.cos(ang), np.sin(ang)]).astype(np.float32)
    ang = 2 * np.pi * (np.arange(16)[:, None] * lanes[None, :]) / PHI
    t_lo = np.stack([np.cos(ang), np.sin(ang)]).astype(np.float32)
    k = np.arange(K)
    ang = 2 * np.pi * ((k[:, None] * k[None, :]) % K) / K
    d = np.zeros((80, 80))
    c, s = np.cos(ang), np.sin(ang)
    d[0:66:2, 0:32], d[0:66:2, 64] = c[:, :32], c[:, 32]
    d[0:66:2, 32:64], d[0:66:2, 65] = s[:, :32], s[:, 32]
    d[1:66:2, 0:32], d[1:66:2, 64] = -s[:, :32], -s[:, 32]
    d[1:66:2, 32:64], d[1:66:2, 65] = c[:, :32], c[:, 32]
    return split_host(f_main), split_host(f_last), split_host(w_phi), t_hi, t_lo, split_host(d)


F_MAIN, F_LAST, W_PHI, TW_HI, TW_LO, D_PSI = host_tables()


def split(x):
    hi = x.astype(BF)
    lo = (x - hi.astype(jnp.float32)).astype(BF)
    return hi, lo


def dot(x, y):
    return jnp.dot(x, y, preferred_element_type=jnp.float32)


def dot_nt(x, y):
    return lax.dot_general(x, y, (((1,), (1,)), ((), ())), preferred_element_type=jnp.float32)


def spectra_kernel(
    g_ref, kern_ref, mine_ref, fm_ref, fl_ref, w_ref, th_ref, tl_ref, out_ref,
    s_ref, acc_ref, lt_ref, rt_ref, s1_ref, last_ref, zh_ref, zl_ref,
):
    mine = mine_ref[0]
    slot = lax.broadcasted_iota(jnp.int32, (ROWS, 128), 0) * 128 + lax.broadcasted_iota(
        jnp.int32, (ROWS, 128), 1
    )
    for s in range(4):
        tod = g_ref[s, 0]
        phi = g_ref[s, 1].astype(jnp.int32)
        psi = g_ref[s, 2].astype(jnp.int32)
        off = g_ref[s, 3].astype(jnp.int32)
        cyc = g_ref[s, 4].astype(jnp.int32)
        cnt = g_ref[s, 5].astype(jnp.int32)
        live = (slot < cnt) & (cyc == mine)
        first = jnp.where(phi == 0, PHI - 1, phi - 1)
        b_hi = (first & 511) >> 4
        is_last = psi == 32
        at = pl.ds(s * ROWS, ROWS)
        s_ref[0, at, :] = jnp.where(live, jnp.where(is_last, b_hi, psi), -1).astype(jnp.float32)
        s_ref[1, at, :] = (first >> 9).astype(jnp.float32)
        s_ref[2, at, :] = jnp.where(is_last, 33, b_hi).astype(jnp.float32)
        s_ref[3, at, :] = (first & 15).astype(jnp.float32)
        for t in range(4):
            weight = jnp.zeros((ROWS, 128), jnp.float32)
            for o in range(8):
                weight = jnp.where(off == o, kern_ref[o, t], weight)
            s_ref[4 + t, at, :] = (tod * weight).astype(BF).astype(jnp.float32)

    acc_ref[...] = jnp.zeros_like(acc_ref)
    sub = lax.broadcasted_iota(jnp.int32, (16, 128), 0).astype(jnp.float32).astype(BF)
    zero = jnp.zeros((16, 128), BF)
    one = jnp.ones((16, 128), BF)

    def build(row0):
        for j in range(BLOCK):

            def row(ch):
                v = s_ref[ch, pl.ds(row0 + j, 1), :]
                return jnp.broadcast_to(v, (16, 128)).astype(BF)

            n_hi, n_lo, m_hi, m_lo = row(0), row(1), row(2), row(3)
            a0, a1, a2, a3 = row(4), row(5), row(6), row(7)
            ones = jnp.where(n_lo == sub, one, zero)
            d = sub - m_lo
            main = jnp.where(
                d == 0.0, a0, jnp.where(d == 1.0, a1, jnp.where(d == 2.0, a2, jnp.where(d == 3.0, a3, zero)))
            )
            spill = jnp.where(
                d == -15.0, a1, jnp.where(d == -14.0, a2, jnp.where(d == -13.0, a3, zero))
            )
            at = pl.ds(j * 128, 128)
            for h in range(32):
                lt_ref[h * 16 : (h + 1) * 16, at] = jnp.where(n_hi == float(h), ones, zero)
            before = None
            for h in range(35):
                here = m_hi == float(h)
                rest = zero if before is None else jnp.where(before, spill, zero)
                rt_ref[h * 16 : (h + 1) * 16, at] = jnp.where(here, main, rest)
                before = here

    def step(i, base):
        build(base + i * BLOCK)
        acc_ref[...] += dot_nt(rt_ref[...], lt_ref[...])
        return base

    for s in range(4):
        count = jnp.max(g_ref[s, 5, 0:8, :]).astype(jnp.int32)
        lax.fori_loop(0, (count + BLOCK * 128 - 1) // (BLOCK * 128), step, s * ROWS)

    lane = lax.broadcasted_iota(jnp.int32, (16, 1024), 1) & 31
    lane = lane.astype(jnp.float32).astype(BF)
    for q in range(32):
        keep = lane == float(q)
        for part in range(2):
            s1_ref[part, q * 16 : (q + 1) * 16, :] = jnp.where(
                keep, fm_ref[part], jnp.zeros((16, 1024), BF)
            )

    def chunk(r0, at):
        tile = acc_ref[r0 : r0 + 16, (at // 8) * 128 : (at // 8) * 128 + 128]
        shift = (at % 8) * 16
        return tile if shift == 0 else pltpu.roll(tile, 128 - shift, 1)

    for h in range(33):
        tile = jnp.zeros((16, 128), jnp.float32)
        if h < 32:
            tile = tile + chunk(528, h)
        if h > 0:
            tile = tile + chunk(544, h - 1)
        last_ref[h * 16 : (h + 1) * 16, :] = tile

    def first_stage(r0, rows):
        at = pl.ds(r0, rows)
        xh, xl = split(acc_ref[at, :])
        y = dot(xh, s1_ref[0]) + dot(xl, s1_ref[0]) + dot(xh, s1_ref[1])
        xh, xl = split(last_ref[at, :])
        y_last = dot(xh, fl_ref[0]) + dot(xl, fl_ref[0]) + dot(xh, fl_ref[1])
        out = []
        for i in range(rows // 16):
            h = r0 // 16 + i
            ch, sh = th_ref[0, h : h + 1, :], th_ref[1, h : h + 1, :]
            cw = ch * tl_ref[0] - sh * tl_ref[1]
            sw = sh * tl_ref[0] + ch * tl_ref[1]
            at = slice(i * 16, (i + 1) * 16)
            yr = jnp.concatenate([y[at, :512], y_last[at, :128]], 1)
            yi = jnp.concatenate([y[at, 512:], y_last[at, 128:]], 1)
            out.append((yr * cw + yi * sw, yi * cw - yr * sw))
        return out

    halo = first_stage(512, 16)[0]
    for r0 in range(0, 512, 128):
        for i, (zr, zi) in enumerate(first_stage(r0, 128)):
            if r0 == 0 and i == 0:
                zr, zi = zr + halo[0], zi + halo[1]
            rh, rl = split(zr)
            ih, il = split(zi)
            at = slice(r0 + i * 16, r0 + (i + 1) * 16)
            for g in range(5):
                take = slice(g * 128, (g + 1) * 128)
                zh_ref[at, g * 256 : g * 256 + 128] = rh[:, take]
                zh_ref[at, g * 256 + 128 : g * 256 + 256] = ih[:, take]
                zl_ref[at, g * 256 : g * 256 + 128] = rl[:, take]
                zl_ref[at, g * 256 + 128 : g * 256 + 256] = il[:, take]

    def put(s_to, tile_no, value):
        out_ref[pl.ds(s_to * TILES + tile_no, 32, stride=4 * TILES), :] = value

    for g in range(5):
        take = slice(g * 256, (g + 1) * 256)
        zh, zl = zh_ref[:, take], zl_ref[:, take]
        p = dot(w_ref[0], zh) + dot(w_ref[1], zh) + dot(w_ref[0], zl)
        parts = (p[:160, :128] + p[160:, 128:], p[:160, 128:] - p[160:, :128])
        if g < 4:
            for c in range(2):
                for e in range(5):
                    s_to, t = divmod(e * 4 + g, 5)
                    put(s_to, c * 5 + t, parts[c][e * 32 : (e + 1) * 32])
            continue
        lanes = lax.broadcasted_iota(jnp.int32, (32, 128), 1)
        for s_to in range(4):
            row = jnp.zeros((32, 128), jnp.float32)
            for c in range(2):
                j = 0
                while j < PER_DEV:
                    e, cl = divmod(PER_DEV * s_to + j, 16)
                    length = min(16 - cl, PER_DEV - j)
                    to = 64 * c + j
                    piece = parts[c][e * 32 : (e + 1) * 32]
                    shift = (to - cl) % 128
                    piece = piece if shift == 0 else pltpu.roll(piece, shift, 1)
                    row = jnp.where((lanes >= to) & (lanes < to + length), piece, row)
                    j += length
            put(s_to, 10, row)


def sky_kernel(r_ref, wig_ref, beam_ref, d_ref, out_ref, wbuf, gh_ref, gl_ref, h_ref, bb_ref, sems):
    def fetch(m):
        return pltpu.make_async_copy(wig_ref.at[m], wbuf.at[m], sems.at[m])

    for m in range(PER_DEV):
        fetch(m).start()

    for k in range(K):
        bb_ref[k] = jnp.broadcast_to(beam_ref[:, k : k + 1], (LB, 128))

    def tile(t):
        return r_ref[pl.ds(t, 128, stride=TILES), :].T

    rem = tile(10)
    sub = lax.broadcasted_iota(jnp.int32, (16, 128), 0)
    for t in range(5):
        planes = (tile(t), tile(5 + t))
        for jj in range(4):
            j = t * 4 + jj
            half = slice((j % 2) * 128, (j % 2) * 128 + 128)
            for c in range(2):
                hi, lo = split(planes[c][jj * 32 : (jj + 1) * 32])
                gh_ref[j // 2, c * 32 : (c + 1) * 32, half] = hi
                gl_ref[j // 2, c * 32 : (c + 1) * 32, half] = lo
            extra = jnp.where(sub == 0, rem[j : j + 1], jnp.where(sub == 1, rem[64 + j : 65 + j], 0.0))
            hi, lo = split(extra)
            gh_ref[j // 2, 64:80, half] = hi
            gl_ref[j // 2, 64:80, half] = lo
    for i in range(PER_DEV // 2):
        h = dot(d_ref[0], gh_ref[i]) + dot(d_ref[1], gh_ref[i]) + dot(d_ref[0], gl_ref[i])
        h_ref[2 * i] = h[:, :128]
        h_ref[2 * i + 1] = h[:, 128:]

    ones = jnp.ones((16, 128), BF)

    def order(m, carry):
        fetch(m).wait()
        real = [jnp.zeros((8, 128), jnp.float32)] * 8
        imag = [jnp.zeros((8, 128), jnp.float32)] * 8
        for k in range(K):
            hr = jnp.broadcast_to(h_ref[m, 2 * k : 2 * k + 1, :], (8, 128))
            hi = jnp.broadcast_to(h_ref[m, 2 * k + 1 : 2 * k + 2, :], (8, 128))
            for i in range(8):
                at = slice(i * 8, (i + 1) * 8)
                w = wbuf[m, k, at, :] * bb_ref[k, at, :]
                real[i] = real[i] + w * hr
                imag[i] = imag[i] + w * hi
        both = jnp.concatenate(real + imag, 0)
        hi, lo = split(both)
        tail = (both - hi.astype(jnp.float32) - lo.astype(jnp.float32)).astype(BF)
        res = dot_nt(ones, hi) + dot_nt(ones, lo) + dot_nt(ones, tail)
        out_ref[pl.ds(m, 1), :] = res[0:1]
        return carry

    lax.fori_loop(0, PER_DEV, order, 0)


def vmem():
    return pl.BlockSpec(memory_space=pltpu.VMEM)


def spectra(gathered, kernel, mine):
    return pl.pallas_call(
        spectra_kernel,
        out_shape=jax.ShapeDtypeStruct((128 * TILES, 128), jnp.float32),
        in_specs=[
            vmem(),
            pl.BlockSpec(memory_space=pltpu.SMEM),
            pl.BlockSpec(memory_space=pltpu.SMEM),
            vmem(), vmem(), vmem(), vmem(), vmem(),
        ],
        out_specs=vmem(),
        scratch_shapes=[
            pltpu.VMEM((8, 128, 128), jnp.float32),
            pltpu.VMEM((CELL_ROWS, 512), jnp.float32),
            pltpu.VMEM((512, BLOCK * 128), BF),
            pltpu.VMEM((CELL_ROWS, BLOCK * 128), BF),
            pltpu.VMEM((2, 512, 1024), BF),
            pltpu.VMEM((528, 128), jnp.float32),
            pltpu.VMEM((512, 1280), BF),
            pltpu.VMEM((512, 1280), BF),
        ],
        compiler_params=pltpu.CompilerParams(vmem_limit_bytes=32 << 20),
        name="spectra",
    )(gathered, kernel, mine, F_MAIN, F_LAST, W_PHI, TW_HI, TW_LO)


def sky_of(received, wigner, beam):
    return pl.pallas_call(
        sky_kernel,
        out_shape=jax.ShapeDtypeStruct((PER_DEV, 2 * LB), jnp.float32),
        in_specs=[vmem(), pl.BlockSpec(memory_space=pl.ANY), vmem(), vmem()],
        out_specs=vmem(),
        scratch_shapes=[
            pltpu.VMEM((PER_DEV, K, LB, RT), jnp.float32),
            pltpu.VMEM((PER_DEV // 2, 80, 256), BF),
            pltpu.VMEM((PER_DEV // 2, 80, 256), BF),
            pltpu.VMEM((PER_DEV, 80, 128), jnp.float32),
            pltpu.VMEM((K, LB, 128), jnp.float32),
            pltpu.SemaphoreType.DMA((PER_DEV,)),
        ],
        compiler_params=pltpu.CompilerParams(vmem_limit_bytes=40 << 20),
        name="sky",
    )(received, wigner, beam, D_PSI)


def body(tod, cycle, phi_cell, psi_bin, offset, counts, kernel, wigner, beam):
    rows = [
        x.reshape(ROWS, 128).astype(jnp.float32) for x in (tod, phi_cell, psi_bin, offset, cycle)
    ]
    rows.append(jnp.broadcast_to(counts.astype(jnp.float32), (ROWS, 128)))
    gathered = lax.all_gather(jnp.stack(rows), "samp")
    mine = lax.axis_index("samp").astype(jnp.int32).reshape(1)
    sent = spectra(gathered, kernel, mine)
    received = lax.all_to_all(
        sent.reshape(128, 1, TILES * 128), ("band", "samp"), 0, 0, tiled=True
    ).reshape(128 * TILES, 128)
    return sky_of(received, wigner[0], beam).reshape(1, PER_DEV, 2 * LB)


def solution(mesh):
    split_both = P("band", "samp")
    placed = (split_both,) * 6 + (P(), P("band", "samp", None, None, None), P())
    return jax.shard_map(
        body, mesh=mesh, in_specs=placed, out_specs=P("band", "samp", None), check_vma=False
    )
```

```python
import jax
import jax.numpy as jnp
import numpy as np
from jax import lax
from jax.experimental import pallas as pl
from jax.experimental.pallas import tpu as pltpu
from jax.sharding import PartitionSpec as P


PHI = 8192
K = 33
LB = 64
RT = 128
PER_DEV = 20
ROWS = 32
BLOCK = 4
CELL_ROWS = 560
TILES = 11
BF = jnp.bfloat16


def split_host(x):
    x = np.asarray(x, np.float32)
    hi = x.astype(BF)
    lo = (x - hi.astype(np.float32)).astype(BF)
    return np.stack([hi, lo])


def host_tables():
    a = np.arange(16)
    cl = np.arange(16)
    ang = 2 * np.pi * ((a[:, None] * cl[None, :]) % 16) / 16
    fc, fs = np.cos(ang), -np.sin(ang)
    f_main = np.concatenate([np.repeat(fc, 32, 1), np.repeat(fs, 32, 1)], 1)
    f_last = np.zeros((128, 256))
    f_last[:16, :16] = fc
    f_last[:16, 128:144] = fs
    b = np.arange(512)
    m2 = (5 * np.arange(32)[None, :] + np.arange(5)[:, None]).reshape(-1)
    ang = 2 * np.pi * ((m2[:, None] * b[None, :]) % 512) / 512
    w_phi = np.concatenate([np.cos(ang), np.sin(ang)], 0)
    lanes = np.concatenate([np.arange(512) // 32, np.where(np.arange(128) < 16, np.arange(128), 0)])
    ang = 2 * np.pi * (16 * np.arange(33)[:, None] * lanes[None, :]) / PHI
    t_hi = np.stack([np.cos(ang), np.sin(ang)]).astype(np.float32)
    ang = 2 * np.pi * (np.arange(16)[:, None] * lanes[None, :]) / PHI
    t_lo = np.stack([np.cos(ang), np.sin(ang)]).astype(np.float32)
    k = np.arange(K)
    ang = 2 * np.pi * ((k[:, None] * k[None, :]) % K) / K
    d = np.zeros((80, 80))
    c, s = np.cos(ang), np.sin(ang)
    d[0:66:2, 0:32], d[0:66:2, 64] = c[:, :32], c[:, 32]
    d[0:66:2, 32:64], d[0:66:2, 65] = s[:, :32], s[:, 32]
    d[1:66:2, 0:32], d[1:66:2, 64] = -s[:, :32], -s[:, 32]
    d[1:66:2, 32:64], d[1:66:2, 65] = c[:, :32], c[:, 32]
    return split_host(f_main), split_host(f_last), split_host(w_phi), t_hi, t_lo, split_host(d)


F_MAIN, F_LAST, W_PHI, TW_HI, TW_LO, D_PSI = host_tables()


def split(x):
    hi = x.astype(BF)
    lo = (x - hi.astype(jnp.float32)).astype(BF)
    return hi, lo


def dot(x, y):
    return jnp.dot(x, y, preferred_element_type=jnp.float32)


def dot_nt(x, y):
    return lax.dot_general(x, y, (((1,), (1,)), ((), ())), preferred_element_type=jnp.float32)


def sort_kernel(
    tod_h, cyc_h, phi_h, psi_h, off_h, cnt_ref, out_ref,
    tod_ref, int_ref, data_ref, to_ref, o_ref, first_ref, first_s, buf_ref, sems,
):
    copies = [pltpu.make_async_copy(tod_h, tod_ref, sems.at[0])]
    for i, src in enumerate((cyc_h, phi_h, psi_h, off_h)):
        copies.append(pltpu.make_async_copy(src, int_ref.at[i], sems.at[1 + i]))
    for c in copies:
        c.start()
    for c in copies:
        c.wait()
    slot = lax.broadcasted_iota(jnp.int32, (ROWS, 128), 0) * 128 + lax.broadcasted_iota(
        jnp.int32, (ROWS, 128), 1
    )
    cyc = jnp.where(slot < cnt_ref[0, 0], int_ref[0], 4)

    def below(n):
        return (
            lax.broadcasted_iota(jnp.int32, (n, n), 0) < lax.broadcasted_iota(jnp.int32, (n, n), 1)
        ).astype(jnp.float32).astype(BF)

    earlier = below(128)
    rows_before = (
        lax.broadcasted_iota(jnp.int32, (ROWS, ROWS), 1) < lax.broadcasted_iota(jnp.int32, (ROWS, ROWS), 0)
    ).astype(jnp.float32).astype(BF)
    every = jnp.ones((128, 128), BF)
    lane0 = lax.broadcasted_iota(jnp.int32, (ROWS, 128), 1)
    place = jnp.full((ROWS, 128), -1.0, jnp.float32)
    for c in range(4):
        mine = (cyc == c).astype(jnp.float32)
        m = mine.astype(BF)
        total = dot(m, every)
        start = dot(rows_before, total.astype(BF))
        first_ref[c * 40 : c * 40 + 32, :] = start.astype(jnp.int32)
        first_ref[c * 40 + 32 : c * 40 + 40, :] = jnp.broadcast_to(
            (start + total)[31:32].astype(jnp.int32), (8, 128)
        )
        pos = (start + dot(m, earlier)).astype(jnp.int32) & 127
        place = jnp.where(cyc == c, (pos + c * 128).astype(jnp.float32), place)
    to_smem = pltpu.make_async_copy(first_ref, first_s, sems.at[5])
    to_smem.start()
    place = place.astype(jnp.int32)
    to_ref[0] = (place >> 4).astype(jnp.float32)
    to_ref[1] = (place & 15).astype(jnp.float32)

    def channel(i, x):
        data_ref[pl.ds(i, ROWS, stride=8), :] = x

    tod = tod_ref[...]
    hi = tod.astype(BF).astype(jnp.float32)
    mid = (tod - hi).astype(BF).astype(jnp.float32)
    channel(0, hi)
    channel(1, mid)
    channel(2, tod - hi - mid)
    channel(3, (int_ref[1] >> 7).astype(jnp.float32))
    channel(4, (int_ref[1] & 127).astype(jnp.float32))
    channel(5, int_ref[2].astype(jnp.float32))
    channel(6, int_ref[3].astype(jnp.float32))
    channel(7, jnp.zeros((ROWS, 128), jnp.float32))

    sub = lax.broadcasted_iota(jnp.int32, (16, 128), 0).astype(jnp.float32).astype(BF)
    zero = jnp.zeros((16, 128), BF)
    one = jnp.ones((16, 128), BF)

    def route(i, carry):
        hi = jnp.broadcast_to(to_ref[0, pl.ds(i, 1), :], (16, 128)).astype(BF)
        lo = jnp.broadcast_to(to_ref[1, pl.ds(i, 1), :], (16, 128)).astype(BF)
        ones = jnp.where(lo == sub, one, zero)
        chosen = jnp.concatenate([jnp.where(hi == float(h), ones, zero) for h in range(32)], 0)
        row = data_ref[pl.ds(pl.multiple_of(i * 8, 8), 8), :].astype(BF)
        o_ref[pl.ds(pl.multiple_of(i * 8, 8), 8), :] = dot_nt(row, chosen)
        return carry

    lax.fori_loop(0, ROWS, route, 0, unroll=4)
    to_smem.wait()
    lane = lax.broadcasted_iota(jnp.int32, (8, 128), 1)

    def append(i, held):
        out = []
        for c in range(4):
            begin = first_s[c * 40 + i, 0]
            row = begin >> 7
            moved = o_ref[pl.ds(pl.multiple_of(i * 8, 8), 8), c * 128 : (c + 1) * 128]
            same = lane >= (begin & 127)
            full = held[c] + jnp.where(same, moved, 0.0)
            over = jnp.where(same, 0.0, moved)
            at = pl.multiple_of((c * 34 + row) * 8, 8)
            buf_ref[pl.ds(at, 8), :] = full
            buf_ref[pl.ds(at + 8, 8), :] = over
            crossed = (first_s[c * 40 + i + 1, 0] >> 7) > row
            out.append(jnp.where(crossed, over, full))
        return tuple(out)

    lax.fori_loop(0, ROWS, append, (jnp.zeros((8, 128), jnp.float32),) * 4, unroll=4)
    for c in range(4):
        valid = slot < first_s[c * 40 + 32, 0]

        def take(ch):
            return buf_ref[pl.ds(c * 34 * 8 + ch, ROWS, stride=8), :]

        out_ref[c, 0] = jnp.where(valid, take(0) + take(1) + take(2), 0.0)
        out_ref[c, 1] = jnp.where(valid, take(3) * 128.0 + take(4), 0.0)
        out_ref[c, 2] = jnp.where(valid, take(5), -1.0)
        out_ref[c, 3] = jnp.where(valid, take(6), 0.0)


def tables_kernel(
    fm_h, fl_h, th_h, tl_h, kern_h, s1_ref, fl_ref, th_ref, tl_ref, kb_ref, fm_ref, kern_ref, sems
):
    pairs = (
        (fm_h, fm_ref), (fl_h, fl_ref), (th_h, th_ref), (tl_h, tl_ref), (kern_h, kern_ref)
    )
    copies = [pltpu.make_async_copy(a, b, sems.at[i]) for i, (a, b) in enumerate(pairs)]
    for c in copies:
        c.start()
    copies[0].wait()
    lane = lax.broadcasted_iota(jnp.int32, (16, 1024), 1) & 31
    lane = lane.astype(jnp.float32).astype(BF)
    for q in range(32):
        keep = lane == float(q)
        for part in range(2):
            s1_ref[part, q * 16 : (q + 1) * 16, :] = jnp.where(
                keep, fm_ref[part], jnp.zeros((16, 1024), BF)
            )
    for c in copies[1:]:
        c.wait()
    for t in range(4):
        for o in range(8):
            kb_ref[t * 8 + o] = jnp.full((8, 128), kern_ref[t, o], jnp.float32)


def spectra_kernel(
    g_ref, s1_ref, fl_ref, th_ref, tl_ref, kb_ref, w_h, out_ref,
    s_ref, acc_ref, lt_ref, rt_ref, last_ref, zh_ref, zl_ref, w_ref, w_sem,
):
    w_copy = pltpu.make_async_copy(w_h, w_ref, w_sem.at[0])
    w_copy.start()
    ends, skips = [], []
    total = jnp.int32(0)
    s_ref[0, 4 * ROWS : 4 * ROWS + 8, :] = jnp.full((8, 128), -1.0, jnp.float32)
    for ch in range(1, 8):
        s_ref[ch, 4 * ROWS : 4 * ROWS + 8, :] = jnp.zeros((8, 128), jnp.float32)
    for s in range(4):
        tod = g_ref[s, 0]
        phi = g_ref[s, 1].astype(jnp.int32)
        psi = g_ref[s, 2].astype(jnp.int32)
        off = g_ref[s, 3].astype(jnp.int32)
        live = psi >= 0
        count = jnp.sum(live.astype(jnp.float32)).astype(jnp.int32)
        rows = (count + 127) >> 7
        total = total + rows
        ends.append(total)
        skips.append(ROWS - rows)
        first = jnp.where(phi == 0, PHI - 1, phi - 1)
        b_hi = (first & 511) >> 4
        is_last = psi == 32
        at = pl.ds(s * ROWS, ROWS)
        s_ref[0, at, :] = jnp.where(live, jnp.where(is_last, b_hi, psi), -1).astype(jnp.float32)
        s_ref[1, at, :] = (first >> 9).astype(jnp.float32)
        s_ref[2, at, :] = jnp.where(is_last, 33, b_hi).astype(jnp.float32)
        s_ref[3, at, :] = (first & 15).astype(jnp.float32)
        for t in range(4):
            weight = jnp.zeros((ROWS, 128), jnp.float32)
            for o in range(8):
                entry = jnp.concatenate([kb_ref[t * 8 + o]] * (ROWS // 8), 0)
                weight = jnp.where(off == o, entry, weight)
            s_ref[4 + t, at, :] = (tod * weight).astype(BF).astype(jnp.float32)

    acc_ref[...] = jnp.zeros_like(acc_ref)
    sub = lax.broadcasted_iota(jnp.int32, (16, 128), 0).astype(jnp.float32).astype(BF)
    zero = jnp.zeros((16, 128), BF)
    one = jnp.ones((16, 128), BF)

    def build(first):
        for j in range(BLOCK):
            f = first + j
            r = f
            for s in range(4):
                r = r + jnp.where(f >= ends[s], skips[s], 0)
            r = jnp.minimum(r, 4 * ROWS)

            def row(ch):
                v = s_ref[ch, pl.ds(r, 1), :]
                return jnp.broadcast_to(v, (16, 128)).astype(BF)

            n_hi, n_lo, m_hi, m_lo = row(0), row(1), row(2), row(3)
            a0, a1, a2, a3 = row(4), row(5), row(6), row(7)
            ones = jnp.where(n_lo == sub, one, zero)
            d = sub - m_lo
            main = jnp.where(
                d == 0.0, a0, jnp.where(d == 1.0, a1, jnp.where(d == 2.0, a2, jnp.where(d == 3.0, a3, zero)))
            )
            spill = jnp.where(
                d == -15.0, a1, jnp.where(d == -14.0, a2, jnp.where(d == -13.0, a3, zero))
            )
            at = pl.ds(j * 128, 128)
            for h in range(32):
                lt_ref[h * 16 : (h + 1) * 16, at] = jnp.where(n_hi == float(h), ones, zero)
            before = None
            for h in range(35):
                here = m_hi == float(h)
                rest = zero if before is None else jnp.where(before, spill, zero)
                rt_ref[h * 16 : (h + 1) * 16, at] = jnp.where(here, main, rest)
                before = here

    def step(i, carry):
        build(i * BLOCK)
        acc_ref[...] += dot_nt(rt_ref[...], lt_ref[...])
        return carry

    lax.fori_loop(0, (total + BLOCK - 1) // BLOCK, step, 0)

    def chunk(r0, at):
        tile = acc_ref[r0 : r0 + 16, (at // 8) * 128 : (at // 8) * 128 + 128]
        shift = (at % 8) * 16
        return tile if shift == 0 else pltpu.roll(tile, 128 - shift, 1)

    for h in range(33):
        tile = jnp.zeros((16, 128), jnp.float32)
        if h < 32:
            tile = tile + chunk(528, h)
        if h > 0:
            tile = tile + chunk(544, h - 1)
        last_ref[h * 16 : (h + 1) * 16, :] = tile

    def first_stage(r0, rows):
        at = pl.ds(r0, rows)
        xh, xl = split(acc_ref[at, :])
        y = dot(xh, s1_ref[0]) + dot(xl, s1_ref[0]) + dot(xh, s1_ref[1])
        xh, xl = split(last_ref[at, :])
        y_last = dot(xh, fl_ref[0]) + dot(xl, fl_ref[0]) + dot(xh, fl_ref[1])
        out = []
        for i in range(rows // 16):
            h = r0 // 16 + i
            ch, sh = th_ref[0, h : h + 1, :], th_ref[1, h : h + 1, :]
            cw = ch * tl_ref[0] - sh * tl_ref[1]
            sw = sh * tl_ref[0] + ch * tl_ref[1]
            at = slice(i * 16, (i + 1) * 16)
            yr = jnp.concatenate([y[at, :512], y_last[at, :128]], 1)
            yi = jnp.concatenate([y[at, 512:], y_last[at, 128:]], 1)
            out.append((yr * cw + yi * sw, yi * cw - yr * sw))
        return out

    halo = first_stage(512, 16)[0]
    for r0 in range(0, 512, 128):
        for i, (zr, zi) in enumerate(first_stage(r0, 128)):
            if r0 == 0 and i == 0:
                zr, zi = zr + halo[0], zi + halo[1]
            rh, rl = split(zr)
            ih, il = split(zi)
            at = slice(r0 + i * 16, r0 + (i + 1) * 16)
            for g in range(5):
                take = slice(g * 128, (g + 1) * 128)
                zh_ref[at, g * 256 : g * 256 + 128] = rh[:, take]
                zh_ref[at, g * 256 + 128 : g * 256 + 256] = ih[:, take]
                zl_ref[at, g * 256 : g * 256 + 128] = rl[:, take]
                zl_ref[at, g * 256 + 128 : g * 256 + 256] = il[:, take]

    w_copy.wait()

    def put(s_to, tile_no, value):
        out_ref[pl.ds(s_to * TILES + tile_no, 32, stride=4 * TILES), :] = value

    for g in range(5):
        take = slice(g * 256, (g + 1) * 256)
        zh, zl = zh_ref[:, take], zl_ref[:, take]
        p = dot(w_ref[0], zh) + dot(w_ref[1], zh) + dot(w_ref[0], zl)
        parts = (p[:160, :128] + p[160:, 128:], p[:160, 128:] - p[160:, :128])
        if g < 4:
            for c in range(2):
                for e in range(5):
                    s_to, t = divmod(e * 4 + g, 5)
                    put(s_to, c * 5 + t, parts[c][e * 32 : (e + 1) * 32])
            continue
        lanes = lax.broadcasted_iota(jnp.int32, (32, 128), 1)
        for s_to in range(4):
            row = jnp.zeros((32, 128), jnp.float32)
            for c in range(2):
                j = 0
                while j < PER_DEV:
                    e, cl = divmod(PER_DEV * s_to + j, 16)
                    length = min(16 - cl, PER_DEV - j)
                    to = 64 * c + j
                    piece = parts[c][e * 32 : (e + 1) * 32]
                    shift = (to - cl) % 128
                    piece = piece if shift == 0 else pltpu.roll(piece, shift, 1)
                    row = jnp.where((lanes >= to) & (lanes < to + length), piece, row)
                    j += length
            put(s_to, 10, row)


def early_kernel(beam_h, d_h, bb_ref, d_ref, beam_ref, sems):
    copies = (
        pltpu.make_async_copy(beam_h, beam_ref, sems.at[0]),
        pltpu.make_async_copy(d_h, d_ref, sems.at[1]),
    )
    for c in copies:
        c.start()
    for c in copies:
        c.wait()
    beam = beam_ref[...].T
    for k in range(K):
        bb_ref[k] = jnp.broadcast_to(beam[:, k : k + 1], (LB, 128))


def sky_kernel(r_ref, wig_h, bb_ref, d_ref, out_ref, wbuf, gh_ref, gl_ref, h_ref, sems):
    def fetch(m):
        return pltpu.make_async_copy(wig_h.at[m], wbuf.at[m], sems.at[m])

    for m in range(PER_DEV):
        fetch(m).start()

    def tile(t):
        return r_ref[pl.ds(t, 128, stride=TILES), :].T

    rem = tile(10)
    sub = lax.broadcasted_iota(jnp.int32, (16, 128), 0)
    for t in range(5):
        planes = (tile(t), tile(5 + t))
        for jj in range(4):
            j = t * 4 + jj
            half = slice((j % 2) * 128, (j % 2) * 128 + 128)
            for c in range(2):
                hi, lo = split(planes[c][jj * 32 : (jj + 1) * 32])
                gh_ref[j // 2, c * 32 : (c + 1) * 32, half] = hi
                gl_ref[j // 2, c * 32 : (c + 1) * 32, half] = lo
            extra = jnp.where(sub == 0, rem[j : j + 1], jnp.where(sub == 1, rem[64 + j : 65 + j], 0.0))
            hi, lo = split(extra)
            gh_ref[j // 2, 64:80, half] = hi
            gl_ref[j // 2, 64:80, half] = lo
    for i in range(PER_DEV // 2):
        h = dot(d_ref[0], gh_ref[i]) + dot(d_ref[1], gh_ref[i]) + dot(d_ref[0], gl_ref[i])
        h_ref[2 * i] = h[:, :128]
        h_ref[2 * i + 1] = h[:, 128:]

    ones = jnp.ones((16, 128), BF)

    def order(m, carry):
        fetch(m).wait()
        real = [jnp.zeros((8, 128), jnp.float32)] * 8
        imag = [jnp.zeros((8, 128), jnp.float32)] * 8
        for k in range(K):
            hr = jnp.broadcast_to(h_ref[m, 2 * k : 2 * k + 1, :], (8, 128))
            hi = jnp.broadcast_to(h_ref[m, 2 * k + 1 : 2 * k + 2, :], (8, 128))
            for i in range(8):
                at = slice(i * 8, (i + 1) * 8)
                w = wbuf[m, k, at, :] * bb_ref[k, at, :]
                real[i] = real[i] + w * hr
                imag[i] = imag[i] + w * hi
        both = jnp.concatenate(real + imag, 0)
        hi, lo = split(both)
        tail = (both - hi.astype(jnp.float32) - lo.astype(jnp.float32)).astype(BF)
        res = dot_nt(ones, hi) + dot_nt(ones, lo) + dot_nt(ones, tail)
        out_ref[pl.ds(m, 1), :] = res[0:1]
        return carry

    lax.fori_loop(0, PER_DEV, order, 0)


def vmem():
    return pl.BlockSpec(memory_space=pltpu.VMEM)


def hbm():
    return pl.BlockSpec(memory_space=pltpu.HBM)


def stay(*arrays):
    return [pltpu.with_memory_space_constraint(jnp.asarray(x), pltpu.HBM) for x in arrays]


def sort(tod, cycle, phi_cell, psi_bin, offset, counts):
    return pl.pallas_call(
        sort_kernel,
        out_shape=jax.ShapeDtypeStruct((4, 4, ROWS, 128), jnp.float32),
        in_specs=[hbm()] * 5 + [pl.BlockSpec(memory_space=pltpu.SMEM)],
        out_specs=vmem(),
        scratch_shapes=[
            pltpu.VMEM((ROWS, 128), jnp.float32),
            pltpu.VMEM((4, ROWS, 128), jnp.int32),
            pltpu.VMEM((ROWS * 8, 128), jnp.float32),
            pltpu.VMEM((2, ROWS, 128), jnp.float32),
            pltpu.VMEM((ROWS * 8, 512), jnp.float32),
            pltpu.VMEM((160, 128), jnp.int32),
            pltpu.SMEM((160, 128), jnp.int32),
            pltpu.VMEM((4 * 34 * 8, 128), jnp.float32),
            pltpu.SemaphoreType.DMA((6,)),
        ],
        compiler_params=pltpu.CompilerParams(vmem_limit_bytes=8 << 20),
        name="sort",
    )(*stay(tod, cycle, phi_cell, psi_bin, offset), counts)


def tables(kernel):
    shapes = ((2, 512, 1024), F_LAST.shape, TW_HI.shape, TW_LO.shape, (32, 8, 128))
    types = (BF, BF) + (jnp.float32,) * 3
    return pl.pallas_call(
        tables_kernel,
        out_shape=[pltpu.VMEM(s, t) for s, t in zip(shapes, types)],
        in_specs=[hbm()] * 5,
        out_specs=[vmem()] * 5,
        scratch_shapes=[
            pltpu.VMEM((2, 16, 1024), BF),
            pltpu.SMEM((4, 8), jnp.float32),
            pltpu.SemaphoreType.DMA((5,)),
        ],
        compiler_params=pltpu.CompilerParams(vmem_limit_bytes=8 << 20),
        name="tables",
    )(*stay(F_MAIN, F_LAST, TW_HI, TW_LO, kernel))


def spectra(gathered, *consts):
    return pl.pallas_call(
        spectra_kernel,
        out_shape=jax.ShapeDtypeStruct((128 * TILES, 128), jnp.float32),
        in_specs=[vmem()] * 6 + [hbm()],
        out_specs=vmem(),
        scratch_shapes=[
            pltpu.VMEM((8, 4 * ROWS + 8, 128), jnp.float32),
            pltpu.VMEM((CELL_ROWS, 512), jnp.float32),
            pltpu.VMEM((512, BLOCK * 128), BF),
            pltpu.VMEM((CELL_ROWS, BLOCK * 128), BF),
            pltpu.VMEM((528, 128), jnp.float32),
            pltpu.VMEM((512, 1280), BF),
            pltpu.VMEM((512, 1280), BF),
            pltpu.VMEM(W_PHI.shape, BF),
            pltpu.SemaphoreType.DMA((1,)),
        ],
        compiler_params=pltpu.CompilerParams(vmem_limit_bytes=20 << 20),
        name="spectra",
    )(gathered, *consts, *stay(W_PHI))


def early(beam):
    return pl.pallas_call(
        early_kernel,
        out_shape=[pltpu.VMEM((K, LB, 128), jnp.float32), pltpu.VMEM(D_PSI.shape, BF)],
        in_specs=[hbm()] * 2,
        out_specs=[vmem()] * 2,
        scratch_shapes=[pltpu.VMEM((K, LB), jnp.float32), pltpu.SemaphoreType.DMA((2,))],
        compiler_params=pltpu.CompilerParams(vmem_limit_bytes=4 << 20),
        name="early",
    )(*stay(beam, D_PSI))


def sky_of(received, wigner, bb, d):
    return pl.pallas_call(
        sky_kernel,
        out_shape=jax.ShapeDtypeStruct((PER_DEV, 2 * LB), jnp.float32),
        in_specs=[vmem(), hbm(), vmem(), vmem()],
        out_specs=vmem(),
        scratch_shapes=[
            pltpu.VMEM((PER_DEV, K, LB, RT), jnp.float32),
            pltpu.VMEM((PER_DEV // 2, 80, 256), BF),
            pltpu.VMEM((PER_DEV // 2, 80, 256), BF),
            pltpu.VMEM((PER_DEV, 80, 128), jnp.float32),
            pltpu.SemaphoreType.DMA((PER_DEV,)),
        ],
        compiler_params=pltpu.CompilerParams(vmem_limit_bytes=36 << 20),
        name="sky",
    )(received, wigner, bb, d)


def body(tod, cycle, phi_cell, psi_bin, offset, counts, kernel, wigner, beam):
    flat = [x.reshape(ROWS, 128) for x in (tod, cycle, phi_cell, psi_bin, offset)]
    lists = sort(*flat, counts)
    gathered = lax.all_to_all(lists, "samp", 0, 0, tiled=True)
    consts = tables(kernel.T)
    sent = spectra(gathered, *consts)
    received = lax.all_to_all(sent.reshape(128, 1, TILES * 128), ("band", "samp"), 0, 0, tiled=True)
    bb, d = early(beam.T)
    sky = sky_of(received.reshape(128 * TILES, 128), wigner[0], bb, d)
    return sky.reshape(1, PER_DEV, 2 * LB)


def solution(mesh):
    split_both = P("band", "samp")
    placed = (split_both,) * 6 + (P(), P("band", "samp", None, None, None), P())
    return jax.shard_map(
        body, mesh=mesh, in_specs=placed, out_specs=P("band", "samp", None), check_vma=False
    )
```

```python
import jax
import jax.numpy as jnp
import numpy as np
from jax import lax
from jax.experimental import pallas as pl
from jax.experimental.pallas import tpu as pltpu
from jax.sharding import PartitionSpec as P


PHI = 8192
K = 33
LB = 64
RT = 128
PER_DEV = 20
ROWS = 32
BLOCK = 4
CELL_ROWS = 560
TILES = 11
HEAD = 2
WROWS = K * LB
WPAD = WROWS + 8
BF = jnp.bfloat16


def split_host(x):
    x = np.asarray(x, np.float32)
    hi = x.astype(BF)
    lo = (x - hi.astype(np.float32)).astype(BF)
    return np.stack([hi, lo])


def host_tables():
    a = np.arange(16)
    cl = np.arange(16)
    ang = 2 * np.pi * ((a[:, None] * cl[None, :]) % 16) / 16
    fc, fs = np.cos(ang), -np.sin(ang)
    packed = np.concatenate([fc[:, :8], fc[:, 8:9], fs[:, 1:8]], 1)
    f_main = np.repeat(packed, 32, 1)
    f_last = np.zeros((128, 256))
    f_last[:16, :16] = fc
    f_last[:16, 128:144] = fs
    b = np.arange(512)
    m2 = (5 * np.arange(32)[None, :] + np.arange(5)[:, None]).reshape(-1)
    ang = 2 * np.pi * ((m2[:, None] * b[None, :]) % 512) / 512
    w_phi = np.concatenate([np.cos(ang), np.sin(ang)], 0)
    lanes = np.concatenate([np.arange(512) // 32, np.where(np.arange(128) < 16, np.arange(128), 0)])
    ang = 2 * np.pi * (16 * np.arange(33)[:, None] * lanes[None, :]) / PHI
    t_hi = np.stack([np.cos(ang), np.sin(ang)]).astype(np.float32)
    ang = 2 * np.pi * (np.arange(16)[:, None] * lanes[None, :]) / PHI
    t_lo = np.stack([np.cos(ang), np.sin(ang)]).astype(np.float32)
    k = np.arange(K)
    ang = 2 * np.pi * ((k[:, None] * k[None, :]) % K) / K
    d = np.zeros((80, 80))
    c, s = np.cos(ang), np.sin(ang)
    d[0:66:2, 0:32], d[0:66:2, 64] = c[:, :32], c[:, 32]
    d[0:66:2, 32:64], d[0:66:2, 65] = s[:, :32], s[:, 32]
    d[1:66:2, 0:32], d[1:66:2, 64] = -s[:, :32], -s[:, 32]
    d[1:66:2, 32:64], d[1:66:2, 65] = c[:, :32], c[:, 32]
    return split_host(f_main), split_host(f_last), split_host(w_phi), t_hi, t_lo, split_host(d)


F_MAIN, F_LAST, W_PHI, TW_HI, TW_LO, D_PSI = host_tables()


def split(x):
    hi = x.astype(BF)
    lo = (x - hi.astype(jnp.float32)).astype(BF)
    return hi, lo


def dot(x, y):
    return jnp.dot(x, y, preferred_element_type=jnp.float32)


def dot_nt(x, y):
    return lax.dot_general(x, y, (((1,), (1,)), ((), ())), preferred_element_type=jnp.float32)


def sort_kernel(
    tod_h, cyc_h, phi_h, psi_h, off_h, cnt_ref, mine_ref, out0, out1, out2, out3,
    tod_ref, int_ref, data_ref, to_ref, o_ref, first_ref, first_s, buf_ref, sems,
):
    copies = [pltpu.make_async_copy(tod_h, tod_ref, sems.at[0])]
    for i, src in enumerate((cyc_h, phi_h, psi_h, off_h)):
        copies.append(pltpu.make_async_copy(src, int_ref.at[i], sems.at[1 + i]))
    for c in copies:
        c.start()
    for c in copies:
        c.wait()
    slot = lax.broadcasted_iota(jnp.int32, (ROWS, 128), 0) * 128 + lax.broadcasted_iota(
        jnp.int32, (ROWS, 128), 1
    )
    cyc = jnp.where(slot < cnt_ref[0, 0], (int_ref[0] - mine_ref[0]) & 3, 4)

    def below(n):
        return (
            lax.broadcasted_iota(jnp.int32, (n, n), 0) < lax.broadcasted_iota(jnp.int32, (n, n), 1)
        ).astype(jnp.float32).astype(BF)

    earlier = below(128)
    rows_before = (
        lax.broadcasted_iota(jnp.int32, (ROWS, ROWS), 1) < lax.broadcasted_iota(jnp.int32, (ROWS, ROWS), 0)
    ).astype(jnp.float32).astype(BF)
    every = jnp.ones((128, 128), BF)
    lane0 = lax.broadcasted_iota(jnp.int32, (ROWS, 128), 1)
    place = jnp.full((ROWS, 128), -1.0, jnp.float32)
    for c in range(4):
        mine = (cyc == c).astype(jnp.float32)
        m = mine.astype(BF)
        total = dot(m, every)
        start = dot(rows_before, total.astype(BF))
        first_ref[c * 40 : c * 40 + 32, :] = start.astype(jnp.int32)
        first_ref[c * 40 + 32 : c * 40 + 40, :] = jnp.broadcast_to(
            (start + total)[31:32].astype(jnp.int32), (8, 128)
        )
        pos = (start + dot(m, earlier)).astype(jnp.int32) & 127
        place = jnp.where(cyc == c, (pos + c * 128).astype(jnp.float32), place)
    to_smem = pltpu.make_async_copy(first_ref, first_s, sems.at[5])
    to_smem.start()
    place = place.astype(jnp.int32)
    to_ref[0] = (place >> 4).astype(jnp.float32)
    to_ref[1] = (place & 15).astype(jnp.float32)

    def channel(i, x):
        data_ref[pl.ds(i, ROWS, stride=8), :] = x

    tod = tod_ref[...]
    hi = tod.astype(BF).astype(jnp.float32)
    mid = (tod - hi).astype(BF).astype(jnp.float32)
    channel(0, hi)
    channel(1, mid)
    channel(2, tod - hi - mid)
    channel(3, (int_ref[1] >> 7).astype(jnp.float32))
    channel(4, (int_ref[1] & 127).astype(jnp.float32))
    channel(5, int_ref[2].astype(jnp.float32))
    channel(6, int_ref[3].astype(jnp.float32))
    channel(7, jnp.zeros((ROWS, 128), jnp.float32))

    sub = lax.broadcasted_iota(jnp.int32, (16, 128), 0).astype(jnp.float32).astype(BF)
    zero = jnp.zeros((16, 128), BF)
    one = jnp.ones((16, 128), BF)

    def route(i, carry):
        hi = jnp.broadcast_to(to_ref[0, pl.ds(i, 1), :], (16, 128)).astype(BF)
        lo = jnp.broadcast_to(to_ref[1, pl.ds(i, 1), :], (16, 128)).astype(BF)
        ones = jnp.where(lo == sub, one, zero)
        chosen = jnp.concatenate([jnp.where(hi == float(h), ones, zero) for h in range(32)], 0)
        row = data_ref[pl.ds(pl.multiple_of(i * 8, 8), 8), :].astype(BF)
        o_ref[pl.ds(pl.multiple_of(i * 8, 8), 8), :] = dot_nt(row, chosen)
        return carry

    lax.fori_loop(0, ROWS, route, 0, unroll=4)
    to_smem.wait()
    lane = lax.broadcasted_iota(jnp.int32, (8, 128), 1)

    def append(i, held):
        out = []
        for c in range(4):
            begin = first_s[c * 40 + i, 0]
            row = begin >> 7
            moved = o_ref[pl.ds(pl.multiple_of(i * 8, 8), 8), c * 128 : (c + 1) * 128]
            same = lane >= (begin & 127)
            full = held[c] + jnp.where(same, moved, 0.0)
            over = jnp.where(same, 0.0, moved)
            at = pl.multiple_of((c * 34 + row) * 8, 8)
            buf_ref[pl.ds(at, 8), :] = full
            buf_ref[pl.ds(at + 8, 8), :] = over
            crossed = (first_s[c * 40 + i + 1, 0] >> 7) > row
            out.append(jnp.where(crossed, over, full))
        return tuple(out)

    lax.fori_loop(0, ROWS, append, (jnp.zeros((8, 128), jnp.float32),) * 4, unroll=4)
    for c, out_ref in enumerate((out0, out1, out2, out3)):
        valid = slot < first_s[c * 40 + 32, 0]

        def take(ch):
            return buf_ref[pl.ds(c * 34 * 8 + ch, ROWS, stride=8), :]

        out_ref[0] = jnp.where(valid, take(0) + take(1) + take(2), 0.0)
        out_ref[1] = jnp.where(valid, take(3) * 128.0 + take(4), 0.0)
        out_ref[2] = jnp.where(valid, take(5), -1.0)
        out_ref[3] = jnp.where(valid, take(6), 0.0)


def tables_kernel(
    fm_h, fl_h, th_h, tl_h, kern_h, s1_ref, fl_ref, th_ref, tl_ref, kb_ref, fm_ref, kern_ref, sems
):
    pairs = (
        (fm_h, fm_ref), (fl_h, fl_ref), (th_h, th_ref), (tl_h, tl_ref), (kern_h, kern_ref)
    )
    copies = [pltpu.make_async_copy(a, b, sems.at[i]) for i, (a, b) in enumerate(pairs)]
    for c in copies:
        c.start()
    copies[0].wait()
    lane = lax.broadcasted_iota(jnp.int32, (16, 512), 1) & 31
    lane = lane.astype(jnp.float32).astype(BF)
    for q in range(32):
        keep = lane == float(q)
        for part in range(2):
            s1_ref[part, q * 16 : (q + 1) * 16, :] = jnp.where(
                keep, fm_ref[part], jnp.zeros((16, 512), BF)
            )
    for c in copies[1:]:
        c.wait()
    for t in range(4):
        for o in range(8):
            kb_ref[t * 8 + o] = jnp.full((8, 128), kern_ref[t, o], jnp.float32)


def spectra_kernel(
    g0, g1, g2, g3, s1_ref, fl_ref, th_ref, tl_ref, kb_ref, w_h, out_ref,
    s_ref, acc_ref, lt_ref, rt_ref, last_ref, zh_ref, zl_ref, w_ref, w_sem,
):
    w_copy = pltpu.make_async_copy(w_h, w_ref, w_sem.at[0])
    w_copy.start()
    ends, skips = [], []
    total = jnp.int32(0)
    s_ref[0, 4 * ROWS : 4 * ROWS + 8, :] = jnp.full((8, 128), -1.0, jnp.float32)
    for ch in range(1, 8):
        s_ref[ch, 4 * ROWS : 4 * ROWS + 8, :] = jnp.zeros((8, 128), jnp.float32)
    for s, g_ref in enumerate((g0, g1, g2, g3)):
        tod = g_ref[0]
        phi = g_ref[1].astype(jnp.int32)
        psi = g_ref[2].astype(jnp.int32)
        off = g_ref[3].astype(jnp.int32)
        live = psi >= 0
        count = jnp.sum(live.astype(jnp.float32)).astype(jnp.int32)
        rows = (count + 127) >> 7
        total = total + rows
        ends.append(total)
        skips.append(ROWS - rows)
        first = jnp.where(phi == 0, PHI - 1, phi - 1)
        b_hi = (first & 511) >> 4
        is_last = psi == 32
        at = pl.ds(s * ROWS, ROWS)
        s_ref[0, at, :] = jnp.where(live, jnp.where(is_last, b_hi, psi), -1).astype(jnp.float32)
        s_ref[1, at, :] = (first >> 9).astype(jnp.float32)
        s_ref[2, at, :] = jnp.where(is_last, 33, b_hi).astype(jnp.float32)
        s_ref[3, at, :] = (first & 15).astype(jnp.float32)
        for t in range(4):
            weight = jnp.zeros((ROWS, 128), jnp.float32)
            for o in range(8):
                entry = jnp.concatenate([kb_ref[t * 8 + o]] * (ROWS // 8), 0)
                weight = jnp.where(off == o, entry, weight)
            s_ref[4 + t, at, :] = (tod * weight).astype(BF).astype(jnp.float32)

    acc_ref[...] = jnp.zeros_like(acc_ref)
    sub = lax.broadcasted_iota(jnp.int32, (16, 128), 0).astype(jnp.float32).astype(BF)
    zero = jnp.zeros((16, 128), BF)
    one = jnp.ones((16, 128), BF)

    def build(first):
        for j in range(BLOCK):
            f = first + j
            r = f
            for s in range(4):
                r = r + jnp.where(f >= ends[s], skips[s], 0)
            r = jnp.minimum(r, 4 * ROWS)

            def row(ch):
                v = s_ref[ch, pl.ds(r, 1), :]
                return jnp.broadcast_to(v, (16, 128)).astype(BF)

            n_hi, n_lo, m_hi, m_lo = row(0), row(1), row(2), row(3)
            a0, a1, a2, a3 = row(4), row(5), row(6), row(7)
            ones = jnp.where(n_lo == sub, one, zero)
            d = sub - m_lo
            main = jnp.where(
                d == 0.0, a0, jnp.where(d == 1.0, a1, jnp.where(d == 2.0, a2, jnp.where(d == 3.0, a3, zero)))
            )
            spill = jnp.where(
                d == -15.0, a1, jnp.where(d == -14.0, a2, jnp.where(d == -13.0, a3, zero))
            )
            at = pl.ds(j * 128, 128)
            for h in range(32):
                lt_ref[h * 16 : (h + 1) * 16, at] = jnp.where(n_hi == float(h), ones, zero)
            before = None
            for h in range(35):
                here = m_hi == float(h)
                rest = zero if before is None else jnp.where(before, spill, zero)
                rt_ref[h * 16 : (h + 1) * 16, at] = jnp.where(here, main, rest)
                before = here

    def step(i, carry):
        build(i * BLOCK)
        acc_ref[...] += dot_nt(rt_ref[...], lt_ref[...])
        return carry

    lax.fori_loop(0, (total + BLOCK - 1) // BLOCK, step, 0)

    def chunk(r0, at):
        tile = acc_ref[r0 : r0 + 16, (at // 8) * 128 : (at // 8) * 128 + 128]
        shift = (at % 8) * 16
        return tile if shift == 0 else pltpu.roll(tile, 128 - shift, 1)

    for h in range(33):
        tile = jnp.zeros((16, 128), jnp.float32)
        if h < 32:
            tile = tile + chunk(528, h)
        if h > 0:
            tile = tile + chunk(544, h - 1)
        last_ref[h * 16 : (h + 1) * 16, :] = tile

    quarter = lax.broadcasted_iota(jnp.int32, (16, 128), 1) >> 5
    none = jnp.zeros((16, 128), jnp.float32)

    def pick(at0, at2, odd):
        return jnp.where(quarter == 0, at0, jnp.where(quarter == 2, at2, odd))

    def first_stage(r0, rows):
        at = pl.ds(r0, rows)
        xh, xl = split(acc_ref[at, :])
        y = dot(xh, s1_ref[0]) + dot(xl, s1_ref[0]) + dot(xh, s1_ref[1])
        xh, xl = split(last_ref[at, :])
        y_last = dot(xh, fl_ref[0]) + dot(xl, fl_ref[0]) + dot(xh, fl_ref[1])
        out = []
        for i in range(rows // 16):
            h = r0 // 16 + i
            ch, sh = th_ref[0, h : h + 1, :], th_ref[1, h : h + 1, :]
            cw = ch * tl_ref[0] - sh * tl_ref[1]
            sw = sh * tl_ref[0] + ch * tl_ref[1]
            at = slice(i * 16, (i + 1) * 16)
            a0, a1, b0, b1 = (y[at, g * 128 : (g + 1) * 128] for g in range(4))
            ra0, ra1, rb0, rb1 = (pltpu.roll(v, 64, 1) for v in (a0, a1, b0, b1))
            yr = jnp.concatenate(
                [a0, a1, pick(b0, a1, ra1), pick(a1, a0, ra0), y_last[at, :128]], 1
            )
            yi = jnp.concatenate(
                [pick(none, b0, b0), b1, -pick(none, b1, rb1), -pick(b1, b0, rb0), y_last[at, 128:]], 1
            )
            out.append((yr * cw + yi * sw, yi * cw - yr * sw))
        return out

    halo = first_stage(512, 16)[0]
    for r0 in range(0, 512, 128):
        for i, (zr, zi) in enumerate(first_stage(r0, 128)):
            if r0 == 0 and i == 0:
                zr, zi = zr + halo[0], zi + halo[1]
            rh, rl = split(zr)
            ih, il = split(zi)
            at = slice(r0 + i * 16, r0 + (i + 1) * 16)
            for g in range(5):
                take = slice(g * 128, (g + 1) * 128)
                zh_ref[at, g * 256 : g * 256 + 128] = rh[:, take]
                zh_ref[at, g * 256 + 128 : g * 256 + 256] = ih[:, take]
                zl_ref[at, g * 256 : g * 256 + 128] = rl[:, take]
                zl_ref[at, g * 256 + 128 : g * 256 + 256] = il[:, take]

    w_copy.wait()

    def put(s_to, tile_no, value):
        out_ref[pl.ds(s_to * TILES + tile_no, 32, stride=4 * TILES), :] = value

    for g in range(5):
        take = slice(g * 256, (g + 1) * 256)
        zh, zl = zh_ref[:, take], zl_ref[:, take]
        p = dot(w_ref[0], zh) + dot(w_ref[1], zh) + dot(w_ref[0], zl)
        parts = (p[:160, :128] + p[160:, 128:], p[:160, 128:] - p[160:, :128])
        if g < 4:
            for c in range(2):
                for e in range(5):
                    s_to, t = divmod(e * 4 + g, 5)
                    put(s_to, c * 5 + t, parts[c][e * 32 : (e + 1) * 32])
            continue
        lanes = lax.broadcasted_iota(jnp.int32, (32, 128), 1)
        for s_to in range(4):
            row = jnp.zeros((32, 128), jnp.float32)
            for c in range(2):
                j = 0
                while j < PER_DEV:
                    e, cl = divmod(PER_DEV * s_to + j, 16)
                    length = min(16 - cl, PER_DEV - j)
                    to = 64 * c + j
                    piece = parts[c][e * 32 : (e + 1) * 32]
                    shift = (to - cl) % 128
                    piece = piece if shift == 0 else pltpu.roll(piece, shift, 1)
                    row = jnp.where((lanes >= to) & (lanes < to + length), piece, row)
                    j += length
            put(s_to, 10, row)


def early_kernel(wig_h, d_h, head_ref, d_ref, sems):
    copies = [pltpu.make_async_copy(d_h, d_ref, sems.at[HEAD])]
    for m in range(HEAD):
        copies.append(
            pltpu.make_async_copy(wig_h.at[m], head_ref.at[m, pl.ds(0, WROWS)], sems.at[m])
        )
    for c in copies:
        c.start()
    for c in copies:
        c.wait()


def sky_kernel(
    r_ref, wig_h, head_ref, beam_ref, d_ref, out_h, wbuf, bb_ref, gh_ref, gl_ref, h_ref, out_ref, sems, out_sem
):
    def fetch(m):
        return pltpu.make_async_copy(
            wig_h.at[m], wbuf.at[m - HEAD, pl.ds(0, WROWS)], sems.at[m - HEAD]
        )

    for m in range(HEAD, PER_DEV):
        fetch(m).start()

    beam = beam_ref[...].T
    for k in range(K):
        bb_ref[k * LB : (k + 1) * LB, :] = jnp.broadcast_to(beam[:, k : k + 1], (LB, 128))

    def tile(t):
        return r_ref[pl.ds(t, 128, stride=TILES), :].T

    rem = tile(10)
    sub = lax.broadcasted_iota(jnp.int32, (16, 128), 0)
    for t in range(5):
        planes = (tile(t), tile(5 + t))
        for jj in range(4):
            j = t * 4 + jj
            half = slice((j % 2) * 128, (j % 2) * 128 + 128)
            for c in range(2):
                hi, lo = split(planes[c][jj * 32 : (jj + 1) * 32])
                gh_ref[j // 2, c * 32 : (c + 1) * 32, half] = hi
                gl_ref[j // 2, c * 32 : (c + 1) * 32, half] = lo
            extra = jnp.where(sub == 0, rem[j : j + 1], jnp.where(sub == 1, rem[64 + j : 65 + j], 0.0))
            hi, lo = split(extra)
            gh_ref[j // 2, 64:80, half] = hi
            gl_ref[j // 2, 64:80, half] = lo
    for i in range(PER_DEV // 2):
        h = dot(d_ref[0], gh_ref[i]) + dot(d_ref[1], gh_ref[i]) + dot(d_ref[0], gl_ref[i])
        h_ref[2 * i] = h[:, :128]
        h_ref[2 * i + 1] = h[:, 128:]

    ones = jnp.ones((16, 128), BF)

    def orders(m, w_ref, at_m):
        sums = [[jnp.zeros((8, 128), jnp.float32)] * 16 for _ in range(2)]
        for k in range(K):
            h = [
                [
                    jnp.broadcast_to(h_ref[m + n, 2 * k + c : 2 * k + c + 1, :], (8, 128))
                    for c in range(2)
                ]
                for n in range(2)
            ]
            for i in range(8):
                row = k * LB + i * 8
                b = bb_ref[row : row + 8, :]
                for n in range(2):
                    w = w_ref[at_m + n, row : row + 8, :] * b
                    sums[n][i] = sums[n][i] + w * h[n][0]
                    sums[n][8 + i] = sums[n][8 + i] + w * h[n][1]
        for n in range(2):
            both = jnp.concatenate(sums[n], 0)
            hi, lo = split(both)
            tail = (both - hi.astype(jnp.float32) - lo.astype(jnp.float32)).astype(BF)
            res = dot_nt(ones, hi) + dot_nt(ones, lo) + dot_nt(ones, tail)
            out_ref[m + n] = res[0:1]

    for m in range(0, HEAD, 2):
        orders(m, head_ref, m)

    def streamed(i, carry):
        m = HEAD + 2 * i
        fetch(m).wait()
        fetch(m + 1).wait()
        orders(m, wbuf, 2 * i)
        return carry

    lax.fori_loop(0, (PER_DEV - HEAD) // 2, streamed, 0)
    out_copy = pltpu.make_async_copy(out_ref, out_h, out_sem.at[0])
    out_copy.start()
    out_copy.wait()


def vmem():
    return pl.BlockSpec(memory_space=pltpu.VMEM)


def hbm():
    return pl.BlockSpec(memory_space=pltpu.HBM)


def stay(*arrays):
    return [pltpu.with_memory_space_constraint(jnp.asarray(x), pltpu.HBM) for x in arrays]


def sort(tod, cycle, phi_cell, psi_bin, offset, counts, mine):
    return pl.pallas_call(
        sort_kernel,
        out_shape=[jax.ShapeDtypeStruct((4, ROWS, 128), jnp.float32)] * 4,
        in_specs=[hbm()] * 5 + [pl.BlockSpec(memory_space=pltpu.SMEM)] * 2,
        out_specs=[vmem()] * 4,
        scratch_shapes=[
            pltpu.VMEM((ROWS, 128), jnp.float32),
            pltpu.VMEM((4, ROWS, 128), jnp.int32),
            pltpu.VMEM((ROWS * 8, 128), jnp.float32),
            pltpu.VMEM((2, ROWS, 128), jnp.float32),
            pltpu.VMEM((ROWS * 8, 512), jnp.float32),
            pltpu.VMEM((160, 128), jnp.int32),
            pltpu.SMEM((160, 128), jnp.int32),
            pltpu.VMEM((4 * 34 * 8, 128), jnp.float32),
            pltpu.SemaphoreType.DMA((6,)),
        ],
        compiler_params=pltpu.CompilerParams(vmem_limit_bytes=8 << 20),
        name="sort",
    )(*stay(tod, cycle, phi_cell, psi_bin, offset), counts, mine)


def tables(kernel):
    shapes = ((2, 512, 512), F_LAST.shape, TW_HI.shape, TW_LO.shape, (32, 8, 128))
    types = (BF, BF) + (jnp.float32,) * 3
    return pl.pallas_call(
        tables_kernel,
        out_shape=[pltpu.VMEM(s, t) for s, t in zip(shapes, types)],
        in_specs=[hbm()] * 5,
        out_specs=[vmem()] * 5,
        scratch_shapes=[
            pltpu.VMEM((2, 16, 512), BF),
            pltpu.SMEM((4, 8), jnp.float32),
            pltpu.SemaphoreType.DMA((5,)),
        ],
        compiler_params=pltpu.CompilerParams(vmem_limit_bytes=8 << 20),
        name="tables",
    )(*stay(F_MAIN, F_LAST, TW_HI, TW_LO, kernel))


def spectra(lists, *consts):
    return pl.pallas_call(
        spectra_kernel,
        out_shape=jax.ShapeDtypeStruct((128 * TILES, 128), jnp.float32),
        in_specs=[vmem()] * 9 + [hbm()],
        out_specs=vmem(),
        scratch_shapes=[
            pltpu.VMEM((8, 4 * ROWS + 8, 128), jnp.float32),
            pltpu.VMEM((CELL_ROWS, 512), jnp.float32),
            pltpu.VMEM((512, BLOCK * 128), BF),
            pltpu.VMEM((CELL_ROWS, BLOCK * 128), BF),
            pltpu.VMEM((528, 128), jnp.float32),
            pltpu.VMEM((512, 1280), BF),
            pltpu.VMEM((512, 1280), BF),
            pltpu.VMEM(W_PHI.shape, BF),
            pltpu.SemaphoreType.DMA((1,)),
        ],
        compiler_params=pltpu.CompilerParams(vmem_limit_bytes=20 << 20),
        name="spectra",
    )(*lists, *consts, *stay(W_PHI))


def early(wigner):
    return pl.pallas_call(
        early_kernel,
        out_shape=[pltpu.VMEM((HEAD, WPAD, RT), jnp.float32), pltpu.VMEM(D_PSI.shape, BF)],
        in_specs=[hbm()] * 2,
        out_specs=[vmem()] * 2,
        scratch_shapes=[pltpu.SemaphoreType.DMA((HEAD + 1,))],
        compiler_params=pltpu.CompilerParams(vmem_limit_bytes=4 << 20),
        name="early",
    )(*stay(wigner, D_PSI))


def sky_of(received, wigner, head, beam, d):
    return pl.pallas_call(
        sky_kernel,
        out_shape=pltpu.HBM((PER_DEV, 1, 2 * LB), jnp.float32),
        in_specs=[vmem(), hbm(), vmem(), vmem(), vmem()],
        out_specs=hbm(),
        scratch_shapes=[
            pltpu.VMEM((PER_DEV - HEAD, WPAD, RT), jnp.float32),
            pltpu.VMEM((WROWS, 128), jnp.float32),
            pltpu.VMEM((PER_DEV // 2, 80, 256), BF),
            pltpu.VMEM((PER_DEV // 2, 80, 256), BF),
            pltpu.VMEM((PER_DEV, 80, 128), jnp.float32),
            pltpu.VMEM((PER_DEV, 1, 2 * LB), jnp.float32),
            pltpu.SemaphoreType.DMA((PER_DEV - HEAD,)),
            pltpu.SemaphoreType.DMA((1,)),
        ],
        compiler_params=pltpu.CompilerParams(vmem_limit_bytes=36 << 20),
        name="sky",
    )(received, *stay(wigner), head, beam, d)


def body(tod, cycle, phi_cell, psi_bin, offset, counts, kernel, wigner, beam):
    flat = [x.reshape(ROWS, 128) for x in (tod, cycle, phi_cell, psi_bin, offset)]
    mine = lax.axis_index("samp").astype(jnp.int32).reshape(1)
    lists = sort(*flat, counts, mine)
    gathered = [lists[0]] + [
        lax.ppermute(lists[d], "samp", [(i, (i + d) % 4) for i in range(4)]) for d in (2, 1, 3)
    ]
    consts = tables(kernel.T)
    sent = spectra(gathered, *consts)
    received = lax.all_to_all(sent.reshape(128, 1, TILES * 128), ("band", "samp"), 0, 0, tiled=True)
    wigner = wigner.reshape(PER_DEV, WROWS, RT)
    head, d = early(wigner)
    sky = sky_of(received.reshape(128 * TILES, 128), wigner, head, beam.T, d)
    return jnp.transpose(sky, (1, 0, 2))


def solution(mesh):
    split_both = P("band", "samp")
    placed = (split_both,) * 6 + (P(), P("band", "samp", None, None, None), P())
    return jax.shard_map(
        body, mesh=mesh, in_specs=placed, out_specs=P("band", "samp", None), check_vma=False
    )
```

```python
import jax
import jax.numpy as jnp
import numpy as np
from jax import lax
from jax.experimental import pallas as pl
from jax.experimental.pallas import tpu as pltpu
from jax.sharding import PartitionSpec as P


PHI = 8192
K = 33
LB = 64
RT = 128
PER_DEV = 20
ROWS = 32
BLOCK = 8
CELL_ROWS = 560
TILES = 11
HEAD = 2
KSTEP = 11
WROWS = K * LB
WPAD = WROWS + 8
BF = jnp.bfloat16


def split_host(x):
    x = np.asarray(x, np.float32)
    hi = x.astype(BF)
    lo = (x - hi.astype(np.float32)).astype(BF)
    return np.stack([hi, lo])


def host_tables():
    a = np.arange(16)
    cl = np.arange(16)
    ang = 2 * np.pi * ((a[:, None] * cl[None, :]) % 16) / 16
    fc, fs = np.cos(ang), -np.sin(ang)
    packed = np.concatenate([fc[:, :8], fc[:, 8:9], fs[:, 1:8]], 1)
    f_main = np.repeat(packed, 32, 1)
    f_last = np.zeros((128, 256))
    f_last[:16, :16] = fc
    f_last[:16, 128:144] = fs
    b = np.arange(512)
    m2 = (5 * np.arange(32)[None, :] + np.arange(5)[:, None]).reshape(-1)
    ang = 2 * np.pi * ((m2[:, None] * b[None, :]) % 512) / 512
    w_phi = np.concatenate([np.cos(ang), np.sin(ang)], 0)
    lanes = np.concatenate([np.arange(512) // 32, np.where(np.arange(128) < 16, np.arange(128), 0)])
    ang = 2 * np.pi * (16 * np.arange(33)[:, None] * lanes[None, :]) / PHI
    t_hi = np.stack([np.cos(ang), np.sin(ang)]).astype(np.float32)
    ang = 2 * np.pi * (np.arange(16)[:, None] * lanes[None, :]) / PHI
    t_lo = np.stack([np.cos(ang), np.sin(ang)]).astype(np.float32)
    k = np.arange(K)
    ang = 2 * np.pi * ((k[:, None] * k[None, :]) % K) / K
    d = np.zeros((80, 80))
    c, s = np.cos(ang), np.sin(ang)
    d[0:66:2, 0:32], d[0:66:2, 64] = c[:, :32], c[:, 32]
    d[0:66:2, 32:64], d[0:66:2, 65] = s[:, :32], s[:, 32]
    d[1:66:2, 0:32], d[1:66:2, 64] = -s[:, :32], -s[:, 32]
    d[1:66:2, 32:64], d[1:66:2, 65] = c[:, :32], c[:, 32]
    return split_host(f_main), split_host(f_last), split_host(w_phi), t_hi, t_lo, split_host(d)


F_MAIN, F_LAST, W_PHI, TW_HI, TW_LO, D_PSI = host_tables()


def split(x):
    hi = x.astype(BF)
    lo = (x - hi.astype(jnp.float32)).astype(BF)
    return hi, lo


def dot(x, y):
    return jnp.dot(x, y, preferred_element_type=jnp.float32)


def dot_nt(x, y):
    return lax.dot_general(x, y, (((1,), (1,)), ((), ())), preferred_element_type=jnp.float32)


def sort_kernel(
    tod_h, cyc_h, phi_h, psi_h, off_h, cnt_ref, mine_ref, out0, out1, out2, out3,
    tod_ref, int_ref, data_ref, to_ref, o_ref, first_ref, first_s, buf_ref, sems,
):
    copies = [pltpu.make_async_copy(tod_h, tod_ref, sems.at[0])]
    for i, src in enumerate((cyc_h, phi_h, psi_h, off_h)):
        copies.append(pltpu.make_async_copy(src, int_ref.at[i], sems.at[1 + i]))
    for c in copies:
        c.start()
    for c in copies:
        c.wait()
    slot = lax.broadcasted_iota(jnp.int32, (ROWS, 128), 0) * 128 + lax.broadcasted_iota(
        jnp.int32, (ROWS, 128), 1
    )
    cyc = jnp.where(slot < cnt_ref[0, 0], (int_ref[0] - mine_ref[0]) & 3, 4)

    def below(n):
        return (
            lax.broadcasted_iota(jnp.int32, (n, n), 0) < lax.broadcasted_iota(jnp.int32, (n, n), 1)
        ).astype(jnp.float32).astype(BF)

    earlier = below(128)
    rows_before = (
        lax.broadcasted_iota(jnp.int32, (ROWS, ROWS), 1) < lax.broadcasted_iota(jnp.int32, (ROWS, ROWS), 0)
    ).astype(jnp.float32).astype(BF)
    every = jnp.ones((128, 128), BF)
    lane0 = lax.broadcasted_iota(jnp.int32, (ROWS, 128), 1)
    place = jnp.full((ROWS, 128), -1.0, jnp.float32)
    for c in range(4):
        mine = (cyc == c).astype(jnp.float32)
        m = mine.astype(BF)
        total = dot(m, every)
        start = dot(rows_before, total.astype(BF))
        first_ref[c * 40 : c * 40 + 32, :] = start.astype(jnp.int32)
        first_ref[c * 40 + 32 : c * 40 + 40, :] = jnp.broadcast_to(
            (start + total)[31:32].astype(jnp.int32), (8, 128)
        )
        pos = (start + dot(m, earlier)).astype(jnp.int32) & 127
        place = jnp.where(cyc == c, (pos + c * 128).astype(jnp.float32), place)
    to_smem = pltpu.make_async_copy(first_ref, first_s, sems.at[5])
    to_smem.start()
    place = place.astype(jnp.int32)
    to_ref[0] = (place >> 4).astype(jnp.float32)
    to_ref[1] = (place & 15).astype(jnp.float32)

    def channel(i, x):
        data_ref[pl.ds(i, ROWS, stride=8), :] = x

    tod = tod_ref[...]
    hi = tod.astype(BF).astype(jnp.float32)
    mid = (tod - hi).astype(BF).astype(jnp.float32)
    channel(0, hi)
    channel(1, mid)
    channel(2, tod - hi - mid)
    channel(3, (int_ref[1] >> 7).astype(jnp.float32))
    channel(4, (int_ref[1] & 127).astype(jnp.float32))
    channel(5, int_ref[2].astype(jnp.float32))
    channel(6, int_ref[3].astype(jnp.float32))
    channel(7, jnp.zeros((ROWS, 128), jnp.float32))

    sub = lax.broadcasted_iota(jnp.int32, (16, 128), 0).astype(jnp.float32).astype(BF)
    zero = jnp.zeros((16, 128), BF)
    one = jnp.ones((16, 128), BF)

    def route(i, carry):
        hi = jnp.broadcast_to(to_ref[0, pl.ds(i, 1), :], (16, 128)).astype(BF)
        lo = jnp.broadcast_to(to_ref[1, pl.ds(i, 1), :], (16, 128)).astype(BF)
        ones = jnp.where(lo == sub, one, zero)
        chosen = jnp.concatenate([jnp.where(hi == float(h), ones, zero) for h in range(32)], 0)
        row = data_ref[pl.ds(pl.multiple_of(i * 8, 8), 8), :].astype(BF)
        o_ref[pl.ds(pl.multiple_of(i * 8, 8), 8), :] = dot_nt(row, chosen)
        return carry

    lax.fori_loop(0, ROWS, route, 0, unroll=4)
    to_smem.wait()
    lane = lax.broadcasted_iota(jnp.int32, (8, 128), 1)

    def append(i, held):
        out = []
        for c in range(4):
            begin = first_s[c * 40 + i, 0]
            row = begin >> 7
            moved = o_ref[pl.ds(pl.multiple_of(i * 8, 8), 8), c * 128 : (c + 1) * 128]
            same = lane >= (begin & 127)
            full = held[c] + jnp.where(same, moved, 0.0)
            over = jnp.where(same, 0.0, moved)
            at = pl.multiple_of((c * 34 + row) * 8, 8)
            buf_ref[pl.ds(at, 8), :] = full
            buf_ref[pl.ds(at + 8, 8), :] = over
            crossed = (first_s[c * 40 + i + 1, 0] >> 7) > row
            out.append(jnp.where(crossed, over, full))
        return tuple(out)

    lax.fori_loop(0, ROWS, append, (jnp.zeros((8, 128), jnp.float32),) * 4, unroll=4)
    for c, out_ref in enumerate((out0, out1, out2, out3)):
        valid = slot < first_s[c * 40 + 32, 0]

        def take(ch):
            return buf_ref[pl.ds(c * 34 * 8 + ch, ROWS, stride=8), :]

        out_ref[0] = jnp.where(valid, take(0) + take(1) + take(2), 0.0)
        out_ref[1] = jnp.where(valid, take(3) * 128.0 + take(4), 0.0)
        out_ref[2] = jnp.where(valid, take(5), -1.0)
        out_ref[3] = jnp.where(valid, take(6), 0.0)


def tables_kernel(
    fm_h, fl_h, th_h, tl_h, kern_h, s1_ref, fl_ref, th_ref, tl_ref, kb_ref, fm_ref, kern_ref, sems
):
    pairs = (
        (fm_h, fm_ref), (fl_h, fl_ref), (th_h, th_ref), (tl_h, tl_ref), (kern_h, kern_ref)
    )
    copies = [pltpu.make_async_copy(a, b, sems.at[i]) for i, (a, b) in enumerate(pairs)]
    for c in copies:
        c.start()
    copies[0].wait()
    lane = lax.broadcasted_iota(jnp.int32, (16, 512), 1) & 31
    lane = lane.astype(jnp.float32).astype(BF)
    for q in range(32):
        keep = lane == float(q)
        for part in range(2):
            s1_ref[part, q * 16 : (q + 1) * 16, :] = jnp.where(
                keep, fm_ref[part], jnp.zeros((16, 512), BF)
            )
    for c in copies[1:]:
        c.wait()
    for t in range(4):
        for o in range(8):
            kb_ref[t * 8 + o] = jnp.full((8, 128), kern_ref[t, o], jnp.float32)


def spectra_kernel(
    g0, g1, g2, g3, s1_ref, fl_ref, th_ref, tl_ref, kb_ref, w_h, out_ref,
    s_ref, acc_ref, last_ref, zh_ref, zl_ref, w_ref, w_sem,
):
    w_copy = pltpu.make_async_copy(w_h, w_ref, w_sem.at[0])
    w_copy.start()
    ends, skips = [], []
    total = jnp.int32(0)
    s_ref[0, 4 * ROWS : 4 * ROWS + 8, :] = jnp.full((8, 128), -1.0, jnp.float32)
    for ch in range(1, 8):
        s_ref[ch, 4 * ROWS : 4 * ROWS + 8, :] = jnp.zeros((8, 128), jnp.float32)
    for s, g_ref in enumerate((g0, g1, g2, g3)):
        tod = g_ref[0]
        phi = g_ref[1].astype(jnp.int32)
        psi = g_ref[2].astype(jnp.int32)
        off = g_ref[3].astype(jnp.int32)
        live = psi >= 0
        count = jnp.sum(live.astype(jnp.float32)).astype(jnp.int32)
        rows = (count + 127) >> 7
        total = total + rows
        ends.append(total)
        skips.append(ROWS - rows)
        first = jnp.where(phi == 0, PHI - 1, phi - 1)
        b_hi = (first & 511) >> 4
        is_last = psi == 32
        at = pl.ds(s * ROWS, ROWS)
        s_ref[0, at, :] = jnp.where(live, jnp.where(is_last, b_hi, psi), -1).astype(jnp.float32)
        s_ref[1, at, :] = (first >> 9).astype(jnp.float32)
        s_ref[2, at, :] = jnp.where(is_last, 33, b_hi).astype(jnp.float32)
        s_ref[3, at, :] = (first & 15).astype(jnp.float32)
        for t in range(4):
            weight = jnp.zeros((ROWS, 128), jnp.float32)
            for o in range(8):
                entry = jnp.concatenate([kb_ref[t * 8 + o]] * (ROWS // 8), 0)
                weight = jnp.where(off == o, entry, weight)
            s_ref[4 + t, at, :] = (tod * weight).astype(BF).astype(jnp.float32)

    acc_ref[...] = jnp.zeros_like(acc_ref)
    sub = lax.broadcasted_iota(jnp.int32, (16, 128), 0).astype(jnp.float32).astype(BF)
    zero = jnp.zeros((16, 128), BF)
    one = jnp.ones((16, 128), BF)

    def build(first):
        left, right = [], []
        for j in range(BLOCK):
            f = first + j
            r = f
            for s in range(4):
                r = r + jnp.where(f >= ends[s], skips[s], 0)
            r = jnp.minimum(r, 4 * ROWS)

            def row(ch):
                v = s_ref[ch, pl.ds(r, 1), :]
                return jnp.broadcast_to(v, (16, 128)).astype(BF)

            n_hi, n_lo, m_hi, m_lo = row(0), row(1), row(2), row(3)
            a0, a1, a2, a3 = row(4), row(5), row(6), row(7)
            ones = jnp.where(n_lo == sub, one, zero)
            d = sub - m_lo
            main = jnp.where(
                d == 0.0, a0, jnp.where(d == 1.0, a1, jnp.where(d == 2.0, a2, jnp.where(d == 3.0, a3, zero)))
            )
            spill = jnp.where(
                d == -15.0, a1, jnp.where(d == -14.0, a2, jnp.where(d == -13.0, a3, zero))
            )
            left.append(jnp.concatenate([jnp.where(n_hi == float(h), ones, zero) for h in range(32)], 0))
            here = [m_hi == float(h) for h in range(35)]
            right.append(
                jnp.concatenate(
                    [jnp.where(here[0], main, zero)]
                    + [
                        jnp.where(here[h], main, jnp.where(here[h - 1], spill, zero))
                        for h in range(1, 35)
                    ],
                    0,
                )
            )
        return left, right

    def step(i, carry):
        left, right = build(i * BLOCK)
        total = None
        for j in range(0, BLOCK, 2):
            part = dot_nt(
                jnp.concatenate(right[j : j + 2], 1), jnp.concatenate(left[j : j + 2], 1)
            )
            total = part if total is None else total + part
        acc_ref[...] += total
        return carry

    lax.fori_loop(0, (total + BLOCK - 1) // BLOCK, step, 0)

    def chunk(r0, at):
        tile = acc_ref[r0 : r0 + 16, (at // 8) * 128 : (at // 8) * 128 + 128]
        shift = (at % 8) * 16
        return tile if shift == 0 else pltpu.roll(tile, 128 - shift, 1)

    for h in range(33):
        tile = jnp.zeros((16, 128), jnp.float32)
        if h < 32:
            tile = tile + chunk(528, h)
        if h > 0:
            tile = tile + chunk(544, h - 1)
        last_ref[h * 16 : (h + 1) * 16, :] = tile

    quarter = lax.broadcasted_iota(jnp.int32, (16, 128), 1) >> 5
    none = jnp.zeros((16, 128), jnp.float32)

    def pick(at0, at2, odd):
        return jnp.where(quarter == 0, at0, jnp.where(quarter == 2, at2, odd))

    def first_stage(r0, rows):
        at = pl.ds(r0, rows)
        xh, xl = split(acc_ref[at, :])
        y = dot(xh, s1_ref[0]) + dot(xl, s1_ref[0]) + dot(xh, s1_ref[1])
        xh, xl = split(last_ref[at, :])
        y_last = dot(xh, fl_ref[0]) + dot(xl, fl_ref[0]) + dot(xh, fl_ref[1])
        out = []
        for i in range(rows // 16):
            h = r0 // 16 + i
            ch, sh = th_ref[0, h : h + 1, :], th_ref[1, h : h + 1, :]
            cw = ch * tl_ref[0] - sh * tl_ref[1]
            sw = sh * tl_ref[0] + ch * tl_ref[1]
            at = slice(i * 16, (i + 1) * 16)
            a0, a1, b0, b1 = (y[at, g * 128 : (g + 1) * 128] for g in range(4))
            ra0, ra1, rb0, rb1 = (pltpu.roll(v, 64, 1) for v in (a0, a1, b0, b1))
            yr = jnp.concatenate(
                [a0, a1, pick(b0, a1, ra1), pick(a1, a0, ra0), y_last[at, :128]], 1
            )
            yi = jnp.concatenate(
                [pick(none, b0, b0), b1, -pick(none, b1, rb1), -pick(b1, b0, rb0), y_last[at, 128:]], 1
            )
            out.append((yr * cw + yi * sw, yi * cw - yr * sw))
        return out

    halo = first_stage(512, 16)[0]
    for r0 in range(0, 512, 128):
        for i, (zr, zi) in enumerate(first_stage(r0, 128)):
            if r0 == 0 and i == 0:
                zr, zi = zr + halo[0], zi + halo[1]
            rh, rl = split(zr)
            ih, il = split(zi)
            at = slice(r0 + i * 16, r0 + (i + 1) * 16)
            for g in range(5):
                take = slice(g * 128, (g + 1) * 128)
                zh_ref[at, g * 256 : g * 256 + 128] = rh[:, take]
                zh_ref[at, g * 256 + 128 : g * 256 + 256] = ih[:, take]
                zl_ref[at, g * 256 : g * 256 + 128] = rl[:, take]
                zl_ref[at, g * 256 + 128 : g * 256 + 256] = il[:, take]

    w_copy.wait()

    def put(s_to, tile_no, value):
        out_ref[pl.ds(s_to * TILES + tile_no, 32, stride=4 * TILES), :] = value

    for g in range(5):
        take = slice(g * 256, (g + 1) * 256)
        zh, zl = zh_ref[:, take], zl_ref[:, take]
        p = dot(w_ref[0], zh) + dot(w_ref[1], zh) + dot(w_ref[0], zl)
        parts = (p[:160, :128] + p[160:, 128:], p[:160, 128:] - p[160:, :128])
        if g < 4:
            for c in range(2):
                for e in range(5):
                    s_to, t = divmod(e * 4 + g, 5)
                    put(s_to, c * 5 + t, parts[c][e * 32 : (e + 1) * 32])
            continue
        lanes = lax.broadcasted_iota(jnp.int32, (32, 128), 1)
        for s_to in range(4):
            row = jnp.zeros((32, 128), jnp.float32)
            for c in range(2):
                j = 0
                while j < PER_DEV:
                    e, cl = divmod(PER_DEV * s_to + j, 16)
                    length = min(16 - cl, PER_DEV - j)
                    to = 64 * c + j
                    piece = parts[c][e * 32 : (e + 1) * 32]
                    shift = (to - cl) % 128
                    piece = piece if shift == 0 else pltpu.roll(piece, shift, 1)
                    row = jnp.where((lanes >= to) & (lanes < to + length), piece, row)
                    j += length
            put(s_to, 10, row)


def early_kernel(wig_h, d_h, head_ref, d_ref, sems):
    copies = [pltpu.make_async_copy(d_h, d_ref, sems.at[HEAD])]
    for m in range(HEAD):
        copies.append(
            pltpu.make_async_copy(wig_h.at[m], head_ref.at[m, pl.ds(0, WROWS)], sems.at[m])
        )
    for c in copies:
        c.start()
    for c in copies:
        c.wait()


def sky_kernel(
    r_ref, wig_h, head_ref, beam_ref, d_ref, out_h, wbuf, bb_ref, gh_ref, gl_ref, h_ref, out_ref, sems, out_sem
):
    def fetch(m):
        return pltpu.make_async_copy(
            wig_h.at[m], wbuf.at[m - HEAD, pl.ds(0, WROWS)], sems.at[m - HEAD]
        )

    for m in range(HEAD, PER_DEV):
        fetch(m).start()

    beam = beam_ref[...].T
    for k in range(K):
        bb_ref[k * LB : (k + 1) * LB, :] = jnp.broadcast_to(beam[:, k : k + 1], (LB, 128))

    def tile(t):
        return r_ref[pl.ds(t, 128, stride=TILES), :].T

    rem = tile(10)
    sub = lax.broadcasted_iota(jnp.int32, (16, 128), 0)
    for t in range(5):
        planes = (tile(t), tile(5 + t))
        for jj in range(4):
            j = t * 4 + jj
            half = slice((j % 2) * 128, (j % 2) * 128 + 128)
            for c in range(2):
                hi, lo = split(planes[c][jj * 32 : (jj + 1) * 32])
                gh_ref[j // 2, c * 32 : (c + 1) * 32, half] = hi
                gl_ref[j // 2, c * 32 : (c + 1) * 32, half] = lo
            extra = jnp.where(sub == 0, rem[j : j + 1], jnp.where(sub == 1, rem[64 + j : 65 + j], 0.0))
            hi, lo = split(extra)
            gh_ref[j // 2, 64:80, half] = hi
            gl_ref[j // 2, 64:80, half] = lo
    for i in range(PER_DEV // 2):
        h = dot(d_ref[0], gh_ref[i]) + dot(d_ref[1], gh_ref[i]) + dot(d_ref[0], gl_ref[i])
        h_ref[2 * i] = h[:, :128]
        h_ref[2 * i + 1] = h[:, 128:]

    ones = jnp.ones((16, 128), BF)

    def orders(m, w_ref, at_m):
        def some(kk, sums):
            sums = [list(x) for x in sums]
            for j in range(KSTEP):
                k = kk * KSTEP + j
                base = pl.multiple_of(k * LB, LB)
                h = [
                    [
                        jnp.broadcast_to(h_ref[m + n, pl.ds(2 * k + c, 1), :], (8, 128))
                        for c in range(2)
                    ]
                    for n in range(2)
                ]
                for i in range(8):
                    b = bb_ref[pl.ds(base + i * 8, 8), :]
                    for n in range(2):
                        w = w_ref[at_m + n, pl.ds(base + i * 8, 8), :] * b
                        sums[n][i] = sums[n][i] + w * h[n][0]
                        sums[n][8 + i] = sums[n][8 + i] + w * h[n][1]
            return tuple(tuple(x) for x in sums)

        sums = ((jnp.zeros((8, 128), jnp.float32),) * 16,) * 2
        sums = lax.fori_loop(0, K // KSTEP, some, sums)
        for n in range(2):
            both = jnp.concatenate(sums[n], 0)
            hi, lo = split(both)
            tail = (both - hi.astype(jnp.float32) - lo.astype(jnp.float32)).astype(BF)
            res = dot_nt(ones, hi) + dot_nt(ones, lo) + dot_nt(ones, tail)
            out_ref[m + n] = res[0:1]

    for m in range(0, HEAD, 2):
        orders(m, head_ref, m)

    def streamed(i, carry):
        m = HEAD + 2 * i
        fetch(m).wait()
        fetch(m + 1).wait()
        orders(m, wbuf, 2 * i)
        return carry

    lax.fori_loop(0, (PER_DEV - HEAD) // 2, streamed, 0)
    out_copy = pltpu.make_async_copy(out_ref, out_h, out_sem.at[0])
    out_copy.start()
    out_copy.wait()


def vmem():
    return pl.BlockSpec(memory_space=pltpu.VMEM)


def hbm():
    return pl.BlockSpec(memory_space=pltpu.HBM)


def stay(*arrays):
    return [pltpu.with_memory_space_constraint(jnp.asarray(x), pltpu.HBM) for x in arrays]


def sort(tod, cycle, phi_cell, psi_bin, offset, counts, mine):
    return pl.pallas_call(
        sort_kernel,
        out_shape=[jax.ShapeDtypeStruct((4, ROWS, 128), jnp.float32)] * 4,
        in_specs=[hbm()] * 5 + [pl.BlockSpec(memory_space=pltpu.SMEM)] * 2,
        out_specs=[vmem()] * 4,
        scratch_shapes=[
            pltpu.VMEM((ROWS, 128), jnp.float32),
            pltpu.VMEM((4, ROWS, 128), jnp.int32),
            pltpu.VMEM((ROWS * 8, 128), jnp.float32),
            pltpu.VMEM((2, ROWS, 128), jnp.float32),
            pltpu.VMEM((ROWS * 8, 512), jnp.float32),
            pltpu.VMEM((160, 128), jnp.int32),
            pltpu.SMEM((160, 128), jnp.int32),
            pltpu.VMEM((4 * 34 * 8, 128), jnp.float32),
            pltpu.SemaphoreType.DMA((6,)),
        ],
        compiler_params=pltpu.CompilerParams(vmem_limit_bytes=8 << 20),
        name="sort",
    )(*stay(tod, cycle, phi_cell, psi_bin, offset), counts, mine)


def tables(kernel):
    shapes = ((2, 512, 512), F_LAST.shape, TW_HI.shape, TW_LO.shape, (32, 8, 128))
    types = (BF, BF) + (jnp.float32,) * 3
    return pl.pallas_call(
        tables_kernel,
        out_shape=[pltpu.VMEM(s, t) for s, t in zip(shapes, types)],
        in_specs=[hbm()] * 5,
        out_specs=[vmem()] * 5,
        scratch_shapes=[
            pltpu.VMEM((2, 16, 512), BF),
            pltpu.SMEM((4, 8), jnp.float32),
            pltpu.SemaphoreType.DMA((5,)),
        ],
        compiler_params=pltpu.CompilerParams(vmem_limit_bytes=8 << 20),
        name="tables",
    )(*stay(F_MAIN, F_LAST, TW_HI, TW_LO, kernel))


def spectra(lists, *consts):
    return pl.pallas_call(
        spectra_kernel,
        out_shape=jax.ShapeDtypeStruct((128 * TILES, 128), jnp.float32),
        in_specs=[vmem()] * 9 + [hbm()],
        out_specs=vmem(),
        scratch_shapes=[
            pltpu.VMEM((8, 4 * ROWS + 8, 128), jnp.float32),
            pltpu.VMEM((CELL_ROWS, 512), jnp.float32),
            pltpu.VMEM((528, 128), jnp.float32),
            pltpu.VMEM((512, 1280), BF),
            pltpu.VMEM((512, 1280), BF),
            pltpu.VMEM(W_PHI.shape, BF),
            pltpu.SemaphoreType.DMA((1,)),
        ],
        compiler_params=pltpu.CompilerParams(vmem_limit_bytes=20 << 20),
        name="spectra",
    )(*lists, *consts, *stay(W_PHI))


def early(wigner):
    return pl.pallas_call(
        early_kernel,
        out_shape=[pltpu.VMEM((HEAD, WPAD, RT), jnp.float32), pltpu.VMEM(D_PSI.shape, BF)],
        in_specs=[hbm()] * 2,
        out_specs=[vmem()] * 2,
        scratch_shapes=[pltpu.SemaphoreType.DMA((HEAD + 1,))],
        compiler_params=pltpu.CompilerParams(vmem_limit_bytes=4 << 20),
        name="early",
    )(*stay(wigner, D_PSI))


def sky_of(received, wigner, head, beam, d):
    return pl.pallas_call(
        sky_kernel,
        out_shape=pltpu.HBM((PER_DEV, 1, 2 * LB), jnp.float32),
        in_specs=[vmem(), hbm(), vmem(), vmem(), vmem()],
        out_specs=hbm(),
        scratch_shapes=[
            pltpu.VMEM((PER_DEV - HEAD, WPAD, RT), jnp.float32),
            pltpu.VMEM((WROWS, 128), jnp.float32),
            pltpu.VMEM((PER_DEV // 2, 80, 256), BF),
            pltpu.VMEM((PER_DEV // 2, 80, 256), BF),
            pltpu.VMEM((PER_DEV, 80, 128), jnp.float32),
            pltpu.VMEM((PER_DEV, 1, 2 * LB), jnp.float32),
            pltpu.SemaphoreType.DMA((PER_DEV - HEAD,)),
            pltpu.SemaphoreType.DMA((1,)),
        ],
        compiler_params=pltpu.CompilerParams(vmem_limit_bytes=36 << 20),
        name="sky",
    )(received, *stay(wigner), head, beam, d)


def body(tod, cycle, phi_cell, psi_bin, offset, counts, kernel, wigner, beam):
    flat = [x.reshape(ROWS, 128) for x in (tod, cycle, phi_cell, psi_bin, offset)]
    mine = lax.axis_index("samp").astype(jnp.int32).reshape(1)
    lists = sort(*flat, counts, mine)
    gathered = [lists[0]] + [
        lax.ppermute(lists[d], "samp", [(i, (i + d) % 4) for i in range(4)]) for d in (2, 1, 3)
    ]
    consts = tables(kernel.T)
    sent = spectra(gathered, *consts)
    received = lax.all_to_all(sent.reshape(128, 1, TILES * 128), ("band", "samp"), 0, 0, tiled=True)
    wigner = wigner.reshape(PER_DEV, WROWS, RT)
    head, d = early(wigner)
    sky = sky_of(received.reshape(128 * TILES, 128), wigner, head, beam.T, d)
    return jnp.transpose(sky, (1, 0, 2))


def solution(mesh):
    split_both = P("band", "samp")
    placed = (split_both,) * 6 + (P(), P("band", "samp", None, None, None), P())
    return jax.shard_map(
        body, mesh=mesh, in_specs=placed, out_specs=P("band", "samp", None), check_vma=False
    )
```

```python
import jax
import jax.numpy as jnp
import numpy as np
from jax import lax
from jax.experimental import pallas as pl
from jax.experimental.pallas import tpu as pltpu
from jax.sharding import PartitionSpec as P


PHI = 8192
K = 33
LB = 64
RT = 128
PER_DEV = 20
ROWS = 32
BLOCK = 8
CELL_ROWS = 560
TILES = 11
HEAD = 2
KSTEP = 11
WROWS = K * LB
WPAD = WROWS + 8
BF = jnp.bfloat16


def split_host(x):
    x = np.asarray(x, np.float32)
    hi = x.astype(BF)
    lo = (x - hi.astype(np.float32)).astype(BF)
    return np.stack([hi, lo])


def host_tables():
    a = np.arange(16)
    cl = np.arange(16)
    ang = 2 * np.pi * ((a[:, None] * cl[None, :]) % 16) / 16
    fc, fs = np.cos(ang), -np.sin(ang)
    packed = np.concatenate([fc[:, :8], fc[:, 8:9], fs[:, 1:8]], 1)
    f_main = np.repeat(packed, 32, 1)
    f_last = np.zeros((128, 256))
    f_last[:16, :16] = fc
    f_last[:16, 128:144] = fs
    b = np.arange(256)
    e, i = np.arange(5)[:, None], np.arange(16)[None, :]
    halves = []
    for odd in range(2):
        m2 = (5 * (2 * i + (e + odd) % 2) + e).reshape(-1)
        ang = 2 * np.pi * ((m2[:, None] * b[None, :]) % 512) / 512
        halves.append(np.concatenate([np.cos(ang), np.sin(ang)], 0))
    w_phi = np.stack(halves)
    lanes = np.concatenate([np.arange(512) // 32, np.where(np.arange(128) < 16, np.arange(128), 0)])
    ang = 2 * np.pi * (16 * np.arange(33)[:, None] * lanes[None, :]) / PHI
    t_hi = np.stack([np.cos(ang), np.sin(ang)]).astype(np.float32)
    ang = 2 * np.pi * (np.arange(16)[:, None] * lanes[None, :]) / PHI
    t_lo = np.stack([np.cos(ang), np.sin(ang)]).astype(np.float32)
    k = np.arange(K)
    ang = 2 * np.pi * ((k[:, None] * k[None, :]) % K) / K
    d = np.zeros((80, 80))
    c, s = np.cos(ang), np.sin(ang)
    d[0:66:2, 0:32], d[0:66:2, 64] = c[:, :32], c[:, 32]
    d[0:66:2, 32:64], d[0:66:2, 65] = s[:, :32], s[:, 32]
    d[1:66:2, 0:32], d[1:66:2, 64] = -s[:, :32], -s[:, 32]
    d[1:66:2, 32:64], d[1:66:2, 65] = c[:, :32], c[:, 32]
    return split_host(f_main), split_host(f_last), split_host(w_phi), t_hi, t_lo, split_host(d)


F_MAIN, F_LAST, W_PHI, TW_HI, TW_LO, D_PSI = host_tables()


def split(x):
    hi = x.astype(BF)
    lo = (x - hi.astype(jnp.float32)).astype(BF)
    return hi, lo


def dot(x, y):
    return jnp.dot(x, y, preferred_element_type=jnp.float32)


def dot_nt(x, y):
    return lax.dot_general(x, y, (((1,), (1,)), ((), ())), preferred_element_type=jnp.float32)


def sort_kernel(
    tod_h, cyc_h, phi_h, psi_h, off_h, cnt_ref, mine_ref, out0, out1, out2, out3,
    tod_ref, int_ref, data_ref, to_ref, o_ref, first_ref, first_s, buf_ref, sems,
):
    copies = [pltpu.make_async_copy(tod_h, tod_ref, sems.at[0])]
    for i, src in enumerate((cyc_h, phi_h, psi_h, off_h)):
        copies.append(pltpu.make_async_copy(src, int_ref.at[i], sems.at[1 + i]))
    for c in copies:
        c.start()
    for c in copies:
        c.wait()
    slot = lax.broadcasted_iota(jnp.int32, (ROWS, 128), 0) * 128 + lax.broadcasted_iota(
        jnp.int32, (ROWS, 128), 1
    )
    cyc = jnp.where(slot < cnt_ref[0, 0], (int_ref[0] - mine_ref[0]) & 3, 4)

    def below(n):
        return (
            lax.broadcasted_iota(jnp.int32, (n, n), 0) < lax.broadcasted_iota(jnp.int32, (n, n), 1)
        ).astype(jnp.float32).astype(BF)

    earlier = below(128)
    rows_before = (
        lax.broadcasted_iota(jnp.int32, (ROWS, ROWS), 1) < lax.broadcasted_iota(jnp.int32, (ROWS, ROWS), 0)
    ).astype(jnp.float32).astype(BF)
    every = jnp.ones((128, 128), BF)
    lane0 = lax.broadcasted_iota(jnp.int32, (ROWS, 128), 1)
    row0 = lax.broadcasted_iota(jnp.int32, (ROWS, 128), 0)
    place = jnp.full((ROWS, 128), -1.0, jnp.float32)
    ahead = jnp.zeros((ROWS, 128), jnp.float32)
    starts, shifts = [], []

    def on_lanes(x, shift):
        return jnp.sum(jnp.where(lane0 == row0 + shift, x, 0.0), axis=0, keepdims=True)

    for c in range(4):
        m = (cyc == c).astype(jnp.float32).astype(BF)
        total = dot(m, every)
        start = dot(rows_before, total.astype(BF))
        starts.append(on_lanes(start + total, 1))
        shifts.append(on_lanes(start - ahead, 0))
        place = jnp.where(cyc == c, ahead + dot(m, earlier), place)
        ahead = ahead + total
    first_ref[...] = jnp.concatenate(starts + shifts, 0).astype(jnp.int32)
    to_smem = pltpu.make_async_copy(first_ref, first_s, sems.at[5])
    to_smem.start()
    place = place.astype(jnp.int32)
    to_ref[0] = (place >> 4).astype(jnp.float32)
    to_ref[1] = (place & 15).astype(jnp.float32)

    def channel(i, x):
        data_ref[pl.ds(i, ROWS, stride=8), :] = x

    tod = tod_ref[...]
    hi = tod.astype(BF).astype(jnp.float32)
    mid = (tod - hi).astype(BF).astype(jnp.float32)
    channel(0, hi)
    channel(1, mid)
    channel(2, tod - hi - mid)
    channel(3, (int_ref[1] >> 7).astype(jnp.float32))
    channel(4, (int_ref[1] & 127).astype(jnp.float32))
    channel(5, int_ref[2].astype(jnp.float32))
    channel(6, int_ref[3].astype(jnp.float32))
    channel(7, jnp.zeros((ROWS, 128), jnp.float32))

    sub = lax.broadcasted_iota(jnp.int32, (16, 128), 0).astype(jnp.float32).astype(BF)
    zero = jnp.zeros((16, 128), BF)
    one = jnp.ones((16, 128), BF)

    def route(i, carry):
        hi = jnp.broadcast_to(to_ref[0, pl.ds(i, 1), :], (16, 128)).astype(BF)
        lo = jnp.broadcast_to(to_ref[1, pl.ds(i, 1), :], (16, 128)).astype(BF)
        ones = jnp.where(lo == sub, one, zero)
        chosen = jnp.concatenate([jnp.where(hi == float(h), ones, zero) for h in range(8)], 0)
        row = data_ref[pl.ds(pl.multiple_of(i * 8, 8), 8), :].astype(BF)
        o_ref[pl.ds(pl.multiple_of(i * 8, 8), 8), :] = dot_nt(row, chosen)
        return carry

    lax.fori_loop(0, ROWS, route, 0, unroll=ROWS)
    to_smem.wait()
    lane = lax.broadcasted_iota(jnp.int32, (8, 128), 1)

    def append(i, held):
        out = []
        moved = o_ref[pl.ds(pl.multiple_of(i * 8, 8), 8), :]
        for c in range(4):
            begin = first_s[c, i]
            after = first_s[c, i + 1]
            row = begin >> 7
            here = begin & 127
            end = here + after - begin
            own = pltpu.roll(moved, first_s[4 + c, i] & 127, 1)
            full = held[c] + jnp.where((lane >= here) & (lane < end), own, 0.0)
            over = jnp.where(lane < end - 128, own, 0.0)
            at = pl.multiple_of((c * 34 + row) * 8, 8)
            buf_ref[pl.ds(at, 8), :] = full
            buf_ref[pl.ds(at + 8, 8), :] = over
            out.append(jnp.where((after >> 7) > row, over, full))
        return tuple(out)

    lax.fori_loop(0, ROWS, append, (jnp.zeros((8, 128), jnp.float32),) * 4, unroll=ROWS)
    for c, out_ref in enumerate((out0, out1, out2, out3)):
        valid = slot < first_s[c, ROWS]

        def take(ch):
            return buf_ref[pl.ds(c * 34 * 8 + ch, ROWS, stride=8), :]

        out_ref[0] = jnp.where(valid, take(0) + take(1) + take(2), 0.0)
        out_ref[1] = jnp.where(valid, take(3) * 128.0 + take(4), 0.0)
        out_ref[2] = jnp.where(valid, take(5), -1.0)
        out_ref[3] = jnp.where(valid, take(6), 0.0)


def tables_kernel(
    fm_h, fl_h, th_h, tl_h, kern_h, s1_ref, fl_ref, th_ref, tl_ref, kb_ref, fm_ref, kern_ref, sems
):
    pairs = (
        (fm_h, fm_ref), (fl_h, fl_ref), (th_h, th_ref), (tl_h, tl_ref), (kern_h, kern_ref)
    )
    copies = [pltpu.make_async_copy(a, b, sems.at[i]) for i, (a, b) in enumerate(pairs)]
    for c in copies:
        c.start()
    copies[0].wait()
    lane = lax.broadcasted_iota(jnp.int32, (16, 512), 1) & 31
    lane = lane.astype(jnp.float32).astype(BF)
    for q in range(32):
        keep = lane == float(q)
        for part in range(2):
            s1_ref[part, q * 16 : (q + 1) * 16, :] = jnp.where(
                keep, fm_ref[part], jnp.zeros((16, 512), BF)
            )
    for c in copies[1:]:
        c.wait()
    for t in range(4):
        for o in range(8):
            kb_ref[t * 8 + o] = jnp.full((8, 128), kern_ref[t, o], jnp.float32)


def spectra_kernel(
    g0, g1, g2, g3, s1_ref, fl_ref, th_ref, tl_ref, kb_ref, w_h, out_ref,
    s_ref, acc_ref, last_ref, zh_ref, zl_ref, w_ref, w_sem,
):
    w_copy = pltpu.make_async_copy(w_h, w_ref, w_sem.at[0])
    w_copy.start()
    ends, skips = [], []
    total = jnp.int32(0)
    s_ref[0, 4 * ROWS : 4 * ROWS + 8, :] = jnp.full((8, 128), -1.0, jnp.float32)
    for ch in range(1, 8):
        s_ref[ch, 4 * ROWS : 4 * ROWS + 8, :] = jnp.zeros((8, 128), jnp.float32)
    for s, g_ref in enumerate((g0, g1, g2, g3)):
        tod = g_ref[0]
        phi = g_ref[1].astype(jnp.int32)
        psi = g_ref[2].astype(jnp.int32)
        off = g_ref[3].astype(jnp.int32)
        live = psi >= 0
        count = jnp.sum(live.astype(jnp.float32)).astype(jnp.int32)
        rows = (count + 127) >> 7
        total = total + rows
        ends.append(total)
        skips.append(ROWS - rows)
        first = jnp.where(phi == 0, PHI - 1, phi - 1)
        b_hi = (first & 511) >> 4
        is_last = psi == 32
        at = pl.ds(s * ROWS, ROWS)
        s_ref[0, at, :] = jnp.where(live, jnp.where(is_last, b_hi, psi), -1).astype(jnp.float32)
        s_ref[1, at, :] = (first >> 9).astype(jnp.float32)
        s_ref[2, at, :] = jnp.where(is_last, 33, b_hi).astype(jnp.float32)
        s_ref[3, at, :] = (first & 15).astype(jnp.float32)
        for t in range(4):
            weight = jnp.zeros((ROWS, 128), jnp.float32)
            for o in range(8):
                entry = jnp.concatenate([kb_ref[t * 8 + o]] * (ROWS // 8), 0)
                weight = jnp.where(off == o, entry, weight)
            s_ref[4 + t, at, :] = (tod * weight).astype(BF).astype(jnp.float32)

    acc_ref[...] = jnp.zeros_like(acc_ref)
    sub = lax.broadcasted_iota(jnp.int32, (16, 128), 0).astype(jnp.float32).astype(BF)
    zero = jnp.zeros((16, 128), BF)
    one = jnp.ones((16, 128), BF)

    def build(first):
        left, right = [], []
        for j in range(BLOCK):
            f = first + j
            r = f
            for s in range(4):
                r = r + jnp.where(f >= ends[s], skips[s], 0)
            r = jnp.minimum(r, 4 * ROWS)

            def row(ch):
                v = s_ref[ch, pl.ds(r, 1), :]
                return jnp.broadcast_to(v, (16, 128)).astype(BF)

            n_hi, n_lo, m_hi, m_lo = row(0), row(1), row(2), row(3)
            a0, a1, a2, a3 = row(4), row(5), row(6), row(7)
            ones = jnp.where(n_lo == sub, one, zero)
            d = sub - m_lo
            main = jnp.where(
                d == 0.0, a0, jnp.where(d == 1.0, a1, jnp.where(d == 2.0, a2, jnp.where(d == 3.0, a3, zero)))
            )
            spill = jnp.where(
                d == -15.0, a1, jnp.where(d == -14.0, a2, jnp.where(d == -13.0, a3, zero))
            )
            left.append(jnp.concatenate([jnp.where(n_hi == float(h), ones, zero) for h in range(32)], 0))
            here = [m_hi == float(h) for h in range(35)]
            right.append(
                jnp.concatenate(
                    [jnp.where(here[0], main, zero)]
                    + [
                        jnp.where(here[h], main, jnp.where(here[h - 1], spill, zero))
                        for h in range(1, 35)
                    ],
                    0,
                )
            )
        return left, right

    def step(i, carry):
        left, right = build(i * BLOCK)
        total = None
        for j in range(0, BLOCK, 2):
            part = dot_nt(
                jnp.concatenate(right[j : j + 2], 1), jnp.concatenate(left[j : j + 2], 1)
            )
            total = part if total is None else total + part
        acc_ref[...] += total
        return carry

    lax.fori_loop(0, (total + BLOCK - 1) // BLOCK, step, 0)

    def chunk(r0, at):
        tile = acc_ref[r0 : r0 + 16, (at // 8) * 128 : (at // 8) * 128 + 128]
        shift = (at % 8) * 16
        return tile if shift == 0 else pltpu.roll(tile, 128 - shift, 1)

    for h in range(33):
        tile = jnp.zeros((16, 128), jnp.float32)
        if h < 32:
            tile = tile + chunk(528, h)
        if h > 0:
            tile = tile + chunk(544, h - 1)
        last_ref[h * 16 : (h + 1) * 16, :] = tile

    quarter = lax.broadcasted_iota(jnp.int32, (16, 128), 1) >> 5
    none = jnp.zeros((16, 128), jnp.float32)

    def pick(at0, at2, odd):
        return jnp.where(quarter == 0, at0, jnp.where(quarter == 2, at2, odd))

    def first_stage(r0, rows):
        at = pl.ds(r0, rows)
        xh, xl = split(acc_ref[at, :])
        y = dot(xh, s1_ref[0]) + dot(xl, s1_ref[0]) + dot(xh, s1_ref[1])
        xh, xl = split(last_ref[at, :])
        y_last = dot(xh, fl_ref[0]) + dot(xl, fl_ref[0]) + dot(xh, fl_ref[1])
        out = []
        for i in range(rows // 16):
            h = r0 // 16 + i
            ch, sh = th_ref[0, h : h + 1, :], th_ref[1, h : h + 1, :]
            cw = ch * tl_ref[0] - sh * tl_ref[1]
            sw = sh * tl_ref[0] + ch * tl_ref[1]
            at = slice(i * 16, (i + 1) * 16)
            a0, a1, b0, b1 = (y[at, g * 128 : (g + 1) * 128] for g in range(4))
            ra0, ra1, rb0, rb1 = (pltpu.roll(v, 64, 1) for v in (a0, a1, b0, b1))
            yr = jnp.concatenate(
                [a0, a1, pick(b0, a1, ra1), pick(a1, a0, ra0), y_last[at, :128]], 1
            )
            yi = jnp.concatenate(
                [pick(none, b0, b0), b1, -pick(none, b1, rb1), -pick(b1, b0, rb0), y_last[at, 128:]], 1
            )
            out.append((yr * cw + yi * sw, yi * cw - yr * sw))
        return out

    halo = first_stage(512, 16)[0]
    for r0 in range(0, 256, 128):
        for i, (near, far) in enumerate(zip(first_stage(r0, 128), first_stage(r0 + 256, 128))):
            if r0 == 0 and i == 0:
                near = (near[0] + halo[0], near[1] + halo[1])
            at = slice(r0 + i * 16, r0 + (i + 1) * 16)
            for odd in range(2):
                zr, zi = (n - f if odd else n + f for n, f in zip(near, far))
                rh, rl = split(zr)
                ih, il = split(zi)
                for g in range(5):
                    take = slice(g * 128, (g + 1) * 128)
                    re, im = slice(g * 256, g * 256 + 128), slice(g * 256 + 128, g * 256 + 256)
                    zh_ref[odd, at, re] = rh[:, take]
                    zh_ref[odd, at, im] = ih[:, take]
                    zl_ref[odd, at, re] = rl[:, take]
                    zl_ref[odd, at, im] = il[:, take]

    w_copy.wait()

    def put(s_to, tile_no, half, value):
        first = (4 * half + s_to) * TILES + tile_no
        out_ref[pl.ds(first, 16, stride=8 * TILES), :] = value

    lanes = lax.broadcasted_iota(jnp.int32, (16, 128), 1)
    last_parts = [[[None] * 5 for _ in range(2)] for _ in range(2)]
    for g in range(5):
        take = slice(g * 256, (g + 1) * 256)
        for odd in range(2):
            zh, zl = zh_ref[odd, :, take], zl_ref[odd, :, take]
            p = dot(w_ref[0, odd], zh) + dot(w_ref[1, odd], zh) + dot(w_ref[0, odd], zl)
            parts = (p[:80, :128] + p[80:, 128:], p[:80, 128:] - p[80:, :128])
            if g < 4:
                for c in range(2):
                    for e in range(5):
                        s_to, t = divmod(e * 4 + g, 5)
                        put(s_to, c * 5 + t, (e + odd) % 2, parts[c][e * 16 : (e + 1) * 16])
                continue
            for c in range(2):
                for e in range(5):
                    last_parts[odd][c][e] = parts[c][e * 16 : (e + 1) * 16]
    for s_to in range(4):
        for half in range(2):
            row = jnp.zeros((16, 128), jnp.float32)
            for c in range(2):
                j = 0
                while j < PER_DEV:
                    e, cl = divmod(PER_DEV * s_to + j, 16)
                    length = min(16 - cl, PER_DEV - j)
                    to = 64 * c + j
                    piece = last_parts[(e + half) % 2][c][e]
                    shift = (to - cl) % 128
                    piece = piece if shift == 0 else pltpu.roll(piece, shift, 1)
                    row = jnp.where((lanes >= to) & (lanes < to + length), piece, row)
                    j += length
            put(s_to, 10, half, row)


def early_kernel(wig_h, d_h, head_ref, d_ref, sems):
    copies = [pltpu.make_async_copy(d_h, d_ref, sems.at[HEAD])]
    for m in range(HEAD):
        copies.append(
            pltpu.make_async_copy(wig_h.at[m], head_ref.at[m, pl.ds(0, WROWS)], sems.at[m])
        )
    for c in copies:
        c.start()
    for c in copies:
        c.wait()


def sky_kernel(
    r_ref, wig_h, head_ref, beam_ref, d_ref, out_h, wbuf, bb_ref, gh_ref, gl_ref, h_ref, out_ref, sems, out_sem
):
    def fetch(m):
        return pltpu.make_async_copy(
            wig_h.at[m], wbuf.at[m - HEAD, pl.ds(0, WROWS)], sems.at[m - HEAD]
        )

    for m in range(HEAD, PER_DEV):
        fetch(m).start()

    beam = beam_ref[...].T
    for k in range(K):
        bb_ref[k * LB : (k + 1) * LB, :] = jnp.broadcast_to(beam[:, k : k + 1], (LB, 128))

    def tile(t):
        return r_ref[pl.ds(t, 128, stride=TILES), :].T

    rem = tile(10)
    sub = lax.broadcasted_iota(jnp.int32, (16, 128), 0)
    for t in range(5):
        planes = (tile(t), tile(5 + t))
        for jj in range(4):
            j = t * 4 + jj
            half = slice((j % 2) * 128, (j % 2) * 128 + 128)
            for c in range(2):
                hi, lo = split(planes[c][jj * 32 : (jj + 1) * 32])
                gh_ref[j // 2, c * 32 : (c + 1) * 32, half] = hi
                gl_ref[j // 2, c * 32 : (c + 1) * 32, half] = lo
            extra = jnp.where(sub == 0, rem[j : j + 1], jnp.where(sub == 1, rem[64 + j : 65 + j], 0.0))
            hi, lo = split(extra)
            gh_ref[j // 2, 64:80, half] = hi
            gl_ref[j // 2, 64:80, half] = lo
    for i in range(PER_DEV // 2):
        h = dot(d_ref[0], gh_ref[i]) + dot(d_ref[1], gh_ref[i]) + dot(d_ref[0], gl_ref[i])
        h_ref[2 * i] = h[:, :128]
        h_ref[2 * i + 1] = h[:, 128:]

    ones = jnp.ones((16, 128), BF)

    def orders(m, w_ref, at_m):
        def some(kk, sums):
            sums = [list(x) for x in sums]
            for j in range(KSTEP):
                k = kk * KSTEP + j
                base = pl.multiple_of(k * LB, LB)
                h = [
                    [
                        jnp.broadcast_to(h_ref[m + n, pl.ds(2 * k + c, 1), :], (8, 128))
                        for c in range(2)
                    ]
                    for n in range(2)
                ]
                for i in range(8):
                    b = bb_ref[pl.ds(base + i * 8, 8), :]
                    for n in range(2):
                        w = w_ref[at_m + n, pl.ds(base + i * 8, 8), :] * b
                        sums[n][i] = sums[n][i] + w * h[n][0]
                        sums[n][8 + i] = sums[n][8 + i] + w * h[n][1]
            return tuple(tuple(x) for x in sums)

        sums = ((jnp.zeros((8, 128), jnp.float32),) * 16,) * 2
        sums = lax.fori_loop(0, K // KSTEP, some, sums)
        for n in range(2):
            both = jnp.concatenate(sums[n], 0)
            hi, lo = split(both)
            tail = (both - hi.astype(jnp.float32) - lo.astype(jnp.float32)).astype(BF)
            res = dot_nt(ones, hi) + dot_nt(ones, lo) + dot_nt(ones, tail)
            out_ref[m + n] = res[0:1]

    for m in range(0, HEAD, 2):
        orders(m, head_ref, m)

    def streamed(i, carry):
        m = HEAD + 2 * i
        fetch(m).wait()
        fetch(m + 1).wait()
        orders(m, wbuf, 2 * i)
        return carry

    lax.fori_loop(0, (PER_DEV - HEAD) // 2, streamed, 0)
    out_copy = pltpu.make_async_copy(out_ref, out_h, out_sem.at[0])
    out_copy.start()
    out_copy.wait()


def vmem():
    return pl.BlockSpec(memory_space=pltpu.VMEM)


def hbm():
    return pl.BlockSpec(memory_space=pltpu.HBM)


def stay(*arrays):
    return [pltpu.with_memory_space_constraint(jnp.asarray(x), pltpu.HBM) for x in arrays]


def sort(tod, cycle, phi_cell, psi_bin, offset, counts, mine):
    return pl.pallas_call(
        sort_kernel,
        out_shape=[jax.ShapeDtypeStruct((4, ROWS, 128), jnp.float32)] * 4,
        in_specs=[hbm()] * 5 + [pl.BlockSpec(memory_space=pltpu.SMEM)] * 2,
        out_specs=[vmem()] * 4,
        scratch_shapes=[
            pltpu.VMEM((ROWS, 128), jnp.float32),
            pltpu.VMEM((4, ROWS, 128), jnp.int32),
            pltpu.VMEM((ROWS * 8, 128), jnp.float32),
            pltpu.VMEM((2, ROWS, 128), jnp.float32),
            pltpu.VMEM((ROWS * 8, 128), jnp.float32),
            pltpu.VMEM((8, 128), jnp.int32),
            pltpu.SMEM((8, 128), jnp.int32),
            pltpu.VMEM((4 * 34 * 8, 128), jnp.float32),
            pltpu.SemaphoreType.DMA((6,)),
        ],
        compiler_params=pltpu.CompilerParams(vmem_limit_bytes=8 << 20),
        name="sort",
    )(*stay(tod, cycle, phi_cell, psi_bin, offset), counts, mine)


def tables(kernel):
    shapes = ((2, 512, 512), F_LAST.shape, TW_HI.shape, TW_LO.shape, (32, 8, 128))
    types = (BF, BF) + (jnp.float32,) * 3
    return pl.pallas_call(
        tables_kernel,
        out_shape=[pltpu.VMEM(s, t) for s, t in zip(shapes, types)],
        in_specs=[hbm()] * 5,
        out_specs=[vmem()] * 5,
        scratch_shapes=[
            pltpu.VMEM((2, 16, 512), BF),
            pltpu.SMEM((4, 8), jnp.float32),
            pltpu.SemaphoreType.DMA((5,)),
        ],
        compiler_params=pltpu.CompilerParams(vmem_limit_bytes=8 << 20),
        name="tables",
    )(*stay(F_MAIN, F_LAST, TW_HI, TW_LO, kernel))


def spectra(lists, *consts):
    return pl.pallas_call(
        spectra_kernel,
        out_shape=jax.ShapeDtypeStruct((128 * TILES, 128), jnp.float32),
        in_specs=[vmem()] * 9 + [hbm()],
        out_specs=vmem(),
        scratch_shapes=[
            pltpu.VMEM((8, 4 * ROWS + 8, 128), jnp.float32),
            pltpu.VMEM((CELL_ROWS, 512), jnp.float32),
            pltpu.VMEM((528, 128), jnp.float32),
            pltpu.VMEM((2, 256, 1280), BF),
            pltpu.VMEM((2, 256, 1280), BF),
            pltpu.VMEM(W_PHI.shape, BF),
            pltpu.SemaphoreType.DMA((1,)),
        ],
        compiler_params=pltpu.CompilerParams(vmem_limit_bytes=20 << 20),
        name="spectra",
    )(*lists, *consts, *stay(W_PHI))


def early(wigner):
    return pl.pallas_call(
        early_kernel,
        out_shape=[pltpu.VMEM((HEAD, WPAD, RT), jnp.float32), pltpu.VMEM(D_PSI.shape, BF)],
        in_specs=[hbm()] * 2,
        out_specs=[vmem()] * 2,
        scratch_shapes=[pltpu.SemaphoreType.DMA((HEAD + 1,))],
        compiler_params=pltpu.CompilerParams(vmem_limit_bytes=4 << 20),
        name="early",
    )(*stay(wigner, D_PSI))


def sky_of(received, wigner, head, beam, d):
    return pl.pallas_call(
        sky_kernel,
        out_shape=pltpu.HBM((PER_DEV, 1, 2 * LB), jnp.float32),
        in_specs=[vmem(), hbm(), vmem(), vmem(), vmem()],
        out_specs=hbm(),
        scratch_shapes=[
            pltpu.VMEM((PER_DEV - HEAD, WPAD, RT), jnp.float32),
            pltpu.VMEM((WROWS, 128), jnp.float32),
            pltpu.VMEM((PER_DEV // 2, 80, 256), BF),
            pltpu.VMEM((PER_DEV // 2, 80, 256), BF),
            pltpu.VMEM((PER_DEV, 80, 128), jnp.float32),
            pltpu.VMEM((PER_DEV, 1, 2 * LB), jnp.float32),
            pltpu.SemaphoreType.DMA((PER_DEV - HEAD,)),
            pltpu.SemaphoreType.DMA((1,)),
        ],
        compiler_params=pltpu.CompilerParams(vmem_limit_bytes=36 << 20),
        name="sky",
    )(received, *stay(wigner), head, beam, d)


def body(tod, cycle, phi_cell, psi_bin, offset, counts, kernel, wigner, beam):
    flat = [x.reshape(ROWS, 128) for x in (tod, cycle, phi_cell, psi_bin, offset)]
    mine = lax.axis_index("samp").astype(jnp.int32).reshape(1)
    lists = sort(*flat, counts, mine)
    gathered = [lists[0]] + [
        lax.ppermute(lists[d], "samp", [(i, (i + d) % 4) for i in range(4)]) for d in (2, 1, 3)
    ]
    consts = tables(kernel.T)
    sent = spectra(gathered, *consts)
    received = lax.all_to_all(sent.reshape(128, 1, TILES * 128), ("band", "samp"), 0, 0, tiled=True)
    wigner = wigner.reshape(PER_DEV, WROWS, RT)
    head, d = early(wigner)
    sky = sky_of(received.reshape(128 * TILES, 128), wigner, head, beam.T, d)
    return jnp.transpose(sky, (1, 0, 2))


def solution(mesh):
    split_both = P("band", "samp")
    placed = (split_both,) * 6 + (P(), P("band", "samp", None, None, None), P())
    return jax.shard_map(
        body, mesh=mesh, in_specs=placed, out_specs=P("band", "samp", None), check_vma=False
    )
```

```python
import jax
import jax.numpy as jnp
import numpy as np
from jax import lax
from jax.experimental import pallas as pl
from jax.experimental.pallas import tpu as pltpu
from jax.sharding import PartitionSpec as P


PHI = 8192
K = 33
LB = 64
RT = 128
PER_DEV = 20
ROWS = 32
BLOCK = 8
CELL_ROWS = 560
TILES = 11
HEAD = 2
KSTEP = 11
WROWS = K * LB
WPAD = WROWS + 8
BF = jnp.bfloat16


def split_host(x):
    x = np.asarray(x, np.float32)
    hi = x.astype(BF)
    lo = (x - hi.astype(np.float32)).astype(BF)
    return np.stack([hi, lo])


def host_tables():
    a = np.arange(16)
    cl = np.arange(16)
    ang = 2 * np.pi * ((a[:, None] * cl[None, :]) % 16) / 16
    fc, fs = np.cos(ang), -np.sin(ang)
    packed = np.concatenate([fc[:, :8], fc[:, 8:9], fs[:, 1:8]], 1)
    f_main = np.repeat(packed, 32, 1)
    f_last = np.zeros((128, 256))
    f_last[:16, :16] = fc
    f_last[:16, 128:144] = fs
    b = np.arange(256)
    e, i = np.arange(5)[:, None], np.arange(16)[None, :]
    halves = []
    for odd in range(2):
        m2 = (5 * (2 * i + (e + odd) % 2) + e).reshape(-1)
        ang = 2 * np.pi * ((m2[:, None] * b[None, :]) % 512) / 512
        halves.append(np.concatenate([np.cos(ang), np.sin(ang)], 0))
    w_phi = np.stack(halves)
    lanes = np.concatenate([np.arange(512) // 32, np.where(np.arange(128) < 16, np.arange(128), 0)])
    ang = 2 * np.pi * (16 * np.arange(33)[:, None] * lanes[None, :]) / PHI
    t_hi = np.stack([np.cos(ang), np.sin(ang)]).astype(np.float32)
    ang = 2 * np.pi * (np.arange(16)[:, None] * lanes[None, :]) / PHI
    t_lo = np.stack([np.cos(ang), np.sin(ang)]).astype(np.float32)
    k = np.arange(K)
    ang = 2 * np.pi * ((k[:, None] * k[None, :]) % K) / K
    d = np.zeros((80, 80))
    c, s = np.cos(ang), np.sin(ang)
    d[0:66:2, 0:32], d[0:66:2, 64] = c[:, :32], c[:, 32]
    d[0:66:2, 32:64], d[0:66:2, 65] = s[:, :32], s[:, 32]
    d[1:66:2, 0:32], d[1:66:2, 64] = -s[:, :32], -s[:, 32]
    d[1:66:2, 32:64], d[1:66:2, 65] = c[:, :32], c[:, 32]
    return split_host(f_main), split_host(f_last), split_host(w_phi), t_hi, t_lo, split_host(d)


F_MAIN, F_LAST, W_PHI, TW_HI, TW_LO, D_PSI = host_tables()


def split(x):
    hi = x.astype(BF)
    lo = (x - hi.astype(jnp.float32)).astype(BF)
    return hi, lo


def dot(x, y):
    return jnp.dot(x, y, preferred_element_type=jnp.float32)


def dot_nt(x, y):
    return lax.dot_general(x, y, (((1,), (1,)), ((), ())), preferred_element_type=jnp.float32)


def sort_kernel(
    tod_h, cyc_h, phi_h, psi_h, off_h, cnt_ref, mine_ref, out0, out1, out2, out3,
    tod_ref, int_ref, data_ref, to_ref, o_ref, first_ref, first_s, buf_ref, sems,
):
    copies = [pltpu.make_async_copy(tod_h, tod_ref, sems.at[0])]
    for i, src in enumerate((cyc_h, phi_h, psi_h, off_h)):
        copies.append(pltpu.make_async_copy(src, int_ref.at[i], sems.at[1 + i]))
    for c in copies:
        c.start()
    for c in copies:
        c.wait()
    slot = lax.broadcasted_iota(jnp.int32, (ROWS, 128), 0) * 128 + lax.broadcasted_iota(
        jnp.int32, (ROWS, 128), 1
    )
    cyc = jnp.where(slot < cnt_ref[0, 0], (int_ref[0] - mine_ref[0]) & 3, 4)

    def below(n):
        return (
            lax.broadcasted_iota(jnp.int32, (n, n), 0) < lax.broadcasted_iota(jnp.int32, (n, n), 1)
        ).astype(jnp.float32).astype(BF)

    earlier = below(128)
    rows_before = (
        lax.broadcasted_iota(jnp.int32, (ROWS, ROWS), 1) < lax.broadcasted_iota(jnp.int32, (ROWS, ROWS), 0)
    ).astype(jnp.float32).astype(BF)
    every = jnp.ones((128, 128), BF)
    lane0 = lax.broadcasted_iota(jnp.int32, (ROWS, 128), 1)
    row0 = lax.broadcasted_iota(jnp.int32, (ROWS, 128), 0)
    place = jnp.full((ROWS, 128), -1.0, jnp.float32)
    ahead = jnp.zeros((ROWS, 128), jnp.float32)
    starts, shifts = [], []

    def on_lanes(x, shift):
        return jnp.sum(jnp.where(lane0 == row0 + shift, x, 0.0), axis=0, keepdims=True)

    for c in range(4):
        m = (cyc == c).astype(jnp.float32).astype(BF)
        total = dot(m, every)
        start = dot(rows_before, total.astype(BF))
        starts.append(on_lanes(start + total, 1))
        shifts.append(on_lanes(start - ahead, 0))
        place = jnp.where(cyc == c, ahead + dot(m, earlier), place)
        ahead = ahead + total
    first_ref[...] = jnp.concatenate(starts + shifts, 0).astype(jnp.int32)
    to_smem = pltpu.make_async_copy(first_ref, first_s, sems.at[5])
    to_smem.start()
    place = place.astype(jnp.int32)
    to_ref[0] = (place >> 4).astype(jnp.float32)
    to_ref[1] = (place & 15).astype(jnp.float32)

    def channel(i, x):
        data_ref[pl.ds(i, ROWS, stride=8), :] = x

    tod = tod_ref[...]
    hi = tod.astype(BF).astype(jnp.float32)
    mid = (tod - hi).astype(BF).astype(jnp.float32)
    channel(0, hi)
    channel(1, mid)
    channel(2, tod - hi - mid)
    channel(3, (int_ref[1] >> 7).astype(jnp.float32))
    channel(4, (int_ref[1] & 127).astype(jnp.float32))
    channel(5, int_ref[2].astype(jnp.float32))
    channel(6, int_ref[3].astype(jnp.float32))
    channel(7, jnp.zeros((ROWS, 128), jnp.float32))

    sub = lax.broadcasted_iota(jnp.int32, (16, 128), 0).astype(jnp.float32).astype(BF)
    zero = jnp.zeros((16, 128), BF)
    one = jnp.ones((16, 128), BF)

    def route(i, carry):
        hi = jnp.broadcast_to(to_ref[0, pl.ds(i, 1), :], (16, 128)).astype(BF)
        lo = jnp.broadcast_to(to_ref[1, pl.ds(i, 1), :], (16, 128)).astype(BF)
        ones = jnp.where(lo == sub, one, zero)
        chosen = jnp.concatenate([jnp.where(hi == float(h), ones, zero) for h in range(8)], 0)
        row = data_ref[pl.ds(pl.multiple_of(i * 8, 8), 8), :].astype(BF)
        o_ref[pl.ds(pl.multiple_of(i * 8, 8), 8), :] = dot_nt(row, chosen)
        return carry

    lax.fori_loop(0, ROWS, route, 0, unroll=ROWS)
    to_smem.wait()
    lane = lax.broadcasted_iota(jnp.int32, (8, 128), 1)

    def append(i, held):
        out = []
        moved = o_ref[pl.ds(pl.multiple_of(i * 8, 8), 8), :]
        for c in range(4):
            begin = first_s[c, i]
            after = first_s[c, i + 1]
            row = begin >> 7
            here = begin & 127
            end = here + after - begin
            own = pltpu.roll(moved, first_s[4 + c, i] & 127, 1)
            full = held[c] + jnp.where((lane >= here) & (lane < end), own, 0.0)
            over = jnp.where(lane < end - 128, own, 0.0)
            at = pl.multiple_of((c * 34 + row) * 8, 8)
            buf_ref[pl.ds(at, 8), :] = full
            buf_ref[pl.ds(at + 8, 8), :] = over
            out.append(jnp.where((after >> 7) > row, over, full))
        return tuple(out)

    lax.fori_loop(0, ROWS, append, (jnp.zeros((8, 128), jnp.float32),) * 4, unroll=ROWS)
    for c, out_ref in enumerate((out0, out1, out2, out3)):
        valid = slot < first_s[c, ROWS]

        def take(ch):
            return buf_ref[pl.ds(c * 34 * 8 + ch, ROWS, stride=8), :]

        out_ref[0] = jnp.where(valid, take(0) + take(1) + take(2), 0.0)
        out_ref[1] = jnp.where(valid, take(3) * 128.0 + take(4), 0.0)
        out_ref[2] = jnp.where(valid, take(5), -1.0)
        out_ref[3] = jnp.where(valid, take(6), 0.0)


def prepare(lists, kb_ref, s_ref):
    spare = len(lists) * ROWS
    ends, skips = [], []
    total = jnp.int32(0)
    s_ref[0, spare : spare + 8, :] = jnp.full((8, 128), -1.0, jnp.float32)
    for ch in range(1, 8):
        s_ref[ch, spare : spare + 8, :] = jnp.zeros((8, 128), jnp.float32)
    for s, g_ref in enumerate(lists):
        tod = g_ref[0]
        phi = g_ref[1].astype(jnp.int32)
        psi = g_ref[2].astype(jnp.int32)
        off = g_ref[3].astype(jnp.int32)
        live = psi >= 0
        count = jnp.sum(live.astype(jnp.float32)).astype(jnp.int32)
        rows = (count + 127) >> 7
        total = total + rows
        ends.append(total)
        skips.append(ROWS - rows)
        first = jnp.where(phi == 0, PHI - 1, phi - 1)
        b_hi = (first & 511) >> 4
        is_last = psi == 32
        at = pl.ds(s * ROWS, ROWS)
        s_ref[0, at, :] = jnp.where(live, jnp.where(is_last, b_hi, psi), -1).astype(jnp.float32)
        s_ref[1, at, :] = (first >> 9).astype(jnp.float32)
        s_ref[2, at, :] = jnp.where(is_last, 33, b_hi).astype(jnp.float32)
        s_ref[3, at, :] = (first & 15).astype(jnp.float32)
        for t in range(4):
            weight = jnp.zeros((ROWS, 128), jnp.float32)
            for o in range(8):
                entry = jnp.concatenate([kb_ref[t * 8 + o]] * (ROWS // 8), 0)
                weight = jnp.where(off == o, entry, weight)
            s_ref[4 + t, at, :] = (tod * weight).astype(BF).astype(jnp.float32)
    return ends, skips, total


def deposit(s_ref, acc_ref, ends, skips, total):
    spare = len(ends) * ROWS
    sub = lax.broadcasted_iota(jnp.int32, (16, 128), 0).astype(jnp.float32).astype(BF)
    zero = jnp.zeros((16, 128), BF)
    one = jnp.ones((16, 128), BF)

    def build(first):
        left, right = [], []
        for j in range(BLOCK):
            f = first + j
            r = f
            for s in range(len(ends)):
                r = r + jnp.where(f >= ends[s], skips[s], 0)
            r = jnp.minimum(r, spare)

            def row(ch):
                v = s_ref[ch, pl.ds(r, 1), :]
                return jnp.broadcast_to(v, (16, 128)).astype(BF)

            n_hi, n_lo, m_hi, m_lo = row(0), row(1), row(2), row(3)
            a0, a1, a2, a3 = row(4), row(5), row(6), row(7)
            ones = jnp.where(n_lo == sub, one, zero)
            d = sub - m_lo
            main = jnp.where(
                d == 0.0, a0, jnp.where(d == 1.0, a1, jnp.where(d == 2.0, a2, jnp.where(d == 3.0, a3, zero)))
            )
            spill = jnp.where(
                d == -15.0, a1, jnp.where(d == -14.0, a2, jnp.where(d == -13.0, a3, zero))
            )
            left.append(jnp.concatenate([jnp.where(n_hi == float(h), ones, zero) for h in range(32)], 0))
            here = [m_hi == float(h) for h in range(35)]
            right.append(
                jnp.concatenate(
                    [jnp.where(here[0], main, zero)]
                    + [
                        jnp.where(here[h], main, jnp.where(here[h - 1], spill, zero))
                        for h in range(1, 35)
                    ],
                    0,
                )
            )
        return left, right

    def step(i, carry):
        left, right = build(i * BLOCK)
        sums = None
        for j in range(0, BLOCK, 2):
            part = dot_nt(
                jnp.concatenate(right[j : j + 2], 1), jnp.concatenate(left[j : j + 2], 1)
            )
            sums = part if sums is None else sums + part
        acc_ref[...] += sums
        return carry

    lax.fori_loop(0, (total + BLOCK - 1) // BLOCK, step, 0)


def tables_kernel(
    g_ref, fm_h, fl_h, th_h, tl_h, kern_h, s1_ref, fl_ref, th_ref, tl_ref, kb_ref, acc_ref,
    fm_ref, kern_ref, s_ref, sems,
):
    pairs = (
        (fm_h, fm_ref), (fl_h, fl_ref), (th_h, th_ref), (tl_h, tl_ref), (kern_h, kern_ref)
    )
    copies = [pltpu.make_async_copy(a, b, sems.at[i]) for i, (a, b) in enumerate(pairs)]
    for c in copies:
        c.start()
    copies[4].wait()
    for t in range(4):
        for o in range(8):
            kb_ref[t * 8 + o] = jnp.full((8, 128), kern_ref[t, o], jnp.float32)
    acc_ref[...] = jnp.zeros_like(acc_ref)
    deposit(s_ref, acc_ref, *prepare((g_ref,), kb_ref, s_ref))
    copies[0].wait()
    lane = lax.broadcasted_iota(jnp.int32, (16, 512), 1) & 31
    lane = lane.astype(jnp.float32).astype(BF)
    for q in range(32):
        keep = lane == float(q)
        for part in range(2):
            s1_ref[part, q * 16 : (q + 1) * 16, :] = jnp.where(
                keep, fm_ref[part], jnp.zeros((16, 512), BF)
            )
    for c in copies[1:4]:
        c.wait()


def spectra_kernel(
    g1, g2, g3, s1_ref, fl_ref, th_ref, tl_ref, kb_ref, own_ref, w_h, out_ref,
    s_ref, acc_ref, last_ref, zh_ref, zl_ref, w_ref, w_sem,
):
    w_copy = pltpu.make_async_copy(w_h, w_ref, w_sem.at[0])
    w_copy.start()
    acc_ref[...] = own_ref[...]
    deposit(s_ref, acc_ref, *prepare((g1, g2, g3), kb_ref, s_ref))

    def chunk(r0, at):
        tile = acc_ref[r0 : r0 + 16, (at // 8) * 128 : (at // 8) * 128 + 128]
        shift = (at % 8) * 16
        return tile if shift == 0 else pltpu.roll(tile, 128 - shift, 1)

    for h in range(33):
        tile = jnp.zeros((16, 128), jnp.float32)
        if h < 32:
            tile = tile + chunk(528, h)
        if h > 0:
            tile = tile + chunk(544, h - 1)
        last_ref[h * 16 : (h + 1) * 16, :] = tile

    quarter = lax.broadcasted_iota(jnp.int32, (16, 128), 1) >> 5
    none = jnp.zeros((16, 128), jnp.float32)

    def pick(at0, at2, odd):
        return jnp.where(quarter == 0, at0, jnp.where(quarter == 2, at2, odd))

    def first_stage(r0, rows):
        at = pl.ds(r0, rows)
        xh, xl = split(acc_ref[at, :])
        y = dot(xh, s1_ref[0]) + dot(xl, s1_ref[0]) + dot(xh, s1_ref[1])
        xh, xl = split(last_ref[at, :])
        y_last = dot(xh, fl_ref[0]) + dot(xl, fl_ref[0]) + dot(xh, fl_ref[1])
        out = []
        for i in range(rows // 16):
            h = r0 // 16 + i
            ch, sh = th_ref[0, h : h + 1, :], th_ref[1, h : h + 1, :]
            cw = ch * tl_ref[0] - sh * tl_ref[1]
            sw = sh * tl_ref[0] + ch * tl_ref[1]
            at = slice(i * 16, (i + 1) * 16)
            a0, a1, b0, b1 = (y[at, g * 128 : (g + 1) * 128] for g in range(4))
            ra0, ra1, rb0, rb1 = (pltpu.roll(v, 64, 1) for v in (a0, a1, b0, b1))
            yr = jnp.concatenate(
                [a0, a1, pick(b0, a1, ra1), pick(a1, a0, ra0), y_last[at, :128]], 1
            )
            yi = jnp.concatenate(
                [pick(none, b0, b0), b1, -pick(none, b1, rb1), -pick(b1, b0, rb0), y_last[at, 128:]], 1
            )
            out.append((yr * cw + yi * sw, yi * cw - yr * sw))
        return out

    halo = first_stage(512, 16)[0]
    for r0 in range(0, 256, 128):
        for i, (near, far) in enumerate(zip(first_stage(r0, 128), first_stage(r0 + 256, 128))):
            if r0 == 0 and i == 0:
                near = (near[0] + halo[0], near[1] + halo[1])
            at = slice(r0 + i * 16, r0 + (i + 1) * 16)
            for odd in range(2):
                zr, zi = (n - f if odd else n + f for n, f in zip(near, far))
                rh, rl = split(zr)
                ih, il = split(zi)
                for g in range(5):
                    take = slice(g * 128, (g + 1) * 128)
                    re, im = slice(g * 256, g * 256 + 128), slice(g * 256 + 128, g * 256 + 256)
                    zh_ref[odd, at, re] = rh[:, take]
                    zh_ref[odd, at, im] = ih[:, take]
                    zl_ref[odd, at, re] = rl[:, take]
                    zl_ref[odd, at, im] = il[:, take]

    w_copy.wait()

    def put(s_to, tile_no, half, value):
        first = (4 * half + s_to) * TILES + tile_no
        out_ref[pl.ds(first, 16, stride=8 * TILES), :] = value

    lanes = lax.broadcasted_iota(jnp.int32, (16, 128), 1)
    last_parts = [[[None] * 5 for _ in range(2)] for _ in range(2)]
    for g in range(5):
        take = slice(g * 256, (g + 1) * 256)
        for odd in range(2):
            zh, zl = zh_ref[odd, :, take], zl_ref[odd, :, take]
            p = dot(w_ref[0, odd], zh) + dot(w_ref[1, odd], zh) + dot(w_ref[0, odd], zl)
            parts = (p[:80, :128] + p[80:, 128:], p[:80, 128:] - p[80:, :128])
            if g < 4:
                for c in range(2):
                    for e in range(5):
                        s_to, t = divmod(e * 4 + g, 5)
                        put(s_to, c * 5 + t, (e + odd) % 2, parts[c][e * 16 : (e + 1) * 16])
                continue
            for c in range(2):
                for e in range(5):
                    last_parts[odd][c][e] = parts[c][e * 16 : (e + 1) * 16]
    for s_to in range(4):
        for half in range(2):
            row = jnp.zeros((16, 128), jnp.float32)
            for c in range(2):
                j = 0
                while j < PER_DEV:
                    e, cl = divmod(PER_DEV * s_to + j, 16)
                    length = min(16 - cl, PER_DEV - j)
                    to = 64 * c + j
                    piece = last_parts[(e + half) % 2][c][e]
                    shift = (to - cl) % 128
                    piece = piece if shift == 0 else pltpu.roll(piece, shift, 1)
                    row = jnp.where((lanes >= to) & (lanes < to + length), piece, row)
                    j += length
            put(s_to, 10, half, row)


def early_kernel(wig_h, d_h, head_ref, d_ref, sems):
    copies = [pltpu.make_async_copy(d_h, d_ref, sems.at[HEAD])]
    for m in range(HEAD):
        copies.append(
            pltpu.make_async_copy(wig_h.at[m], head_ref.at[m, pl.ds(0, WROWS)], sems.at[m])
        )
    for c in copies:
        c.start()
    for c in copies:
        c.wait()


def sky_kernel(
    r_ref, wig_h, head_ref, beam_ref, d_ref, out_h, wbuf, bb_ref, gh_ref, gl_ref, h_ref, out_ref, sems, out_sem
):
    def fetch(m):
        return pltpu.make_async_copy(
            wig_h.at[m], wbuf.at[m - HEAD, pl.ds(0, WROWS)], sems.at[m - HEAD]
        )

    for m in range(HEAD, PER_DEV):
        fetch(m).start()

    beam = beam_ref[...].T
    for k in range(K):
        bb_ref[k * LB : (k + 1) * LB, :] = jnp.broadcast_to(beam[:, k : k + 1], (LB, 128))

    def tile(t):
        return r_ref[pl.ds(t, 128, stride=TILES), :].T

    rem = tile(10)
    sub = lax.broadcasted_iota(jnp.int32, (16, 128), 0)
    for t in range(5):
        planes = (tile(t), tile(5 + t))
        for jj in range(4):
            j = t * 4 + jj
            half = slice((j % 2) * 128, (j % 2) * 128 + 128)
            for c in range(2):
                hi, lo = split(planes[c][jj * 32 : (jj + 1) * 32])
                gh_ref[j // 2, c * 32 : (c + 1) * 32, half] = hi
                gl_ref[j // 2, c * 32 : (c + 1) * 32, half] = lo
            extra = jnp.where(sub == 0, rem[j : j + 1], jnp.where(sub == 1, rem[64 + j : 65 + j], 0.0))
            hi, lo = split(extra)
            gh_ref[j // 2, 64:80, half] = hi
            gl_ref[j // 2, 64:80, half] = lo
    for i in range(PER_DEV // 2):
        h = dot(d_ref[0], gh_ref[i]) + dot(d_ref[1], gh_ref[i]) + dot(d_ref[0], gl_ref[i])
        h_ref[2 * i] = h[:, :128]
        h_ref[2 * i + 1] = h[:, 128:]

    ones = jnp.ones((16, 128), BF)

    def orders(m, w_ref, at_m):
        def some(kk, sums):
            sums = [list(x) for x in sums]
            for j in range(KSTEP):
                k = kk * KSTEP + j
                base = pl.multiple_of(k * LB, LB)
                h = [
                    [
                        jnp.broadcast_to(h_ref[m + n, pl.ds(2 * k + c, 1), :], (8, 128))
                        for c in range(2)
                    ]
                    for n in range(2)
                ]
                for i in range(8):
                    b = bb_ref[pl.ds(base + i * 8, 8), :]
                    for n in range(2):
                        w = w_ref[at_m + n, pl.ds(base + i * 8, 8), :] * b
                        sums[n][i] = sums[n][i] + w * h[n][0]
                        sums[n][8 + i] = sums[n][8 + i] + w * h[n][1]
            return tuple(tuple(x) for x in sums)

        sums = ((jnp.zeros((8, 128), jnp.float32),) * 16,) * 2
        sums = lax.fori_loop(0, K // KSTEP, some, sums)
        for n in range(2):
            both = jnp.concatenate(sums[n], 0)
            hi, lo = split(both)
            tail = (both - hi.astype(jnp.float32) - lo.astype(jnp.float32)).astype(BF)
            res = dot_nt(ones, hi) + dot_nt(ones, lo) + dot_nt(ones, tail)
            out_ref[m + n] = res[0:1]

    for m in range(0, HEAD, 2):
        orders(m, head_ref, m)

    def streamed(i, carry):
        m = HEAD + 2 * i
        fetch(m).wait()
        fetch(m + 1).wait()
        orders(m, wbuf, 2 * i)
        return carry

    lax.fori_loop(0, (PER_DEV - HEAD) // 2, streamed, 0)
    out_copy = pltpu.make_async_copy(out_ref, out_h, out_sem.at[0])
    out_copy.start()
    out_copy.wait()


def vmem():
    return pl.BlockSpec(memory_space=pltpu.VMEM)


def hbm():
    return pl.BlockSpec(memory_space=pltpu.HBM)


def stay(*arrays):
    return [pltpu.with_memory_space_constraint(jnp.asarray(x), pltpu.HBM) for x in arrays]


def sort(tod, cycle, phi_cell, psi_bin, offset, counts, mine):
    return pl.pallas_call(
        sort_kernel,
        out_shape=[jax.ShapeDtypeStruct((4, ROWS, 128), jnp.float32)] * 4,
        in_specs=[hbm()] * 5 + [pl.BlockSpec(memory_space=pltpu.SMEM)] * 2,
        out_specs=[vmem()] * 4,
        scratch_shapes=[
            pltpu.VMEM((ROWS, 128), jnp.float32),
            pltpu.VMEM((4, ROWS, 128), jnp.int32),
            pltpu.VMEM((ROWS * 8, 128), jnp.float32),
            pltpu.VMEM((2, ROWS, 128), jnp.float32),
            pltpu.VMEM((ROWS * 8, 128), jnp.float32),
            pltpu.VMEM((8, 128), jnp.int32),
            pltpu.SMEM((8, 128), jnp.int32),
            pltpu.VMEM((4 * 34 * 8, 128), jnp.float32),
            pltpu.SemaphoreType.DMA((6,)),
        ],
        compiler_params=pltpu.CompilerParams(vmem_limit_bytes=8 << 20),
        name="sort",
    )(*stay(tod, cycle, phi_cell, psi_bin, offset), counts, mine)


def tables(own, kernel):
    shapes = ((2, 512, 512), F_LAST.shape, TW_HI.shape, TW_LO.shape, (32, 8, 128), (CELL_ROWS, 512))
    types = (BF, BF) + (jnp.float32,) * 4
    return pl.pallas_call(
        tables_kernel,
        out_shape=[pltpu.VMEM(s, t) for s, t in zip(shapes, types)],
        in_specs=[vmem()] + [hbm()] * 5,
        out_specs=[vmem()] * 6,
        scratch_shapes=[
            pltpu.VMEM((2, 16, 512), BF),
            pltpu.SMEM((4, 8), jnp.float32),
            pltpu.VMEM((8, ROWS + 8, 128), jnp.float32),
            pltpu.SemaphoreType.DMA((5,)),
        ],
        compiler_params=pltpu.CompilerParams(vmem_limit_bytes=16 << 20),
        name="tables",
    )(own, *stay(F_MAIN, F_LAST, TW_HI, TW_LO, kernel))


def spectra(lists, *consts):
    return pl.pallas_call(
        spectra_kernel,
        out_shape=jax.ShapeDtypeStruct((128 * TILES, 128), jnp.float32),
        in_specs=[vmem()] * 9 + [hbm()],
        out_specs=vmem(),
        scratch_shapes=[
            pltpu.VMEM((8, 3 * ROWS + 8, 128), jnp.float32),
            pltpu.VMEM((CELL_ROWS, 512), jnp.float32),
            pltpu.VMEM((528, 128), jnp.float32),
            pltpu.VMEM((2, 256, 1280), BF),
            pltpu.VMEM((2, 256, 1280), BF),
            pltpu.VMEM(W_PHI.shape, BF),
            pltpu.SemaphoreType.DMA((1,)),
        ],
        compiler_params=pltpu.CompilerParams(vmem_limit_bytes=20 << 20),
        name="spectra",
    )(*lists, *consts, *stay(W_PHI))


def early(wigner):
    return pl.pallas_call(
        early_kernel,
        out_shape=[pltpu.VMEM((HEAD, WPAD, RT), jnp.float32), pltpu.VMEM(D_PSI.shape, BF)],
        in_specs=[hbm()] * 2,
        out_specs=[vmem()] * 2,
        scratch_shapes=[pltpu.SemaphoreType.DMA((HEAD + 1,))],
        compiler_params=pltpu.CompilerParams(vmem_limit_bytes=4 << 20),
        name="early",
    )(*stay(wigner, D_PSI))


def sky_of(received, wigner, head, beam, d):
    return pl.pallas_call(
        sky_kernel,
        out_shape=pltpu.HBM((PER_DEV, 1, 2 * LB), jnp.float32),
        in_specs=[vmem(), hbm(), vmem(), vmem(), vmem()],
        out_specs=hbm(),
        scratch_shapes=[
            pltpu.VMEM((PER_DEV - HEAD, WPAD, RT), jnp.float32),
            pltpu.VMEM((WROWS, 128), jnp.float32),
            pltpu.VMEM((PER_DEV // 2, 80, 256), BF),
            pltpu.VMEM((PER_DEV // 2, 80, 256), BF),
            pltpu.VMEM((PER_DEV, 80, 128), jnp.float32),
            pltpu.VMEM((PER_DEV, 1, 2 * LB), jnp.float32),
            pltpu.SemaphoreType.DMA((PER_DEV - HEAD,)),
            pltpu.SemaphoreType.DMA((1,)),
        ],
        compiler_params=pltpu.CompilerParams(vmem_limit_bytes=36 << 20),
        name="sky",
    )(received, *stay(wigner), head, beam, d)


def body(tod, cycle, phi_cell, psi_bin, offset, counts, kernel, wigner, beam):
    flat = [x.reshape(ROWS, 128) for x in (tod, cycle, phi_cell, psi_bin, offset)]
    mine = lax.axis_index("samp").astype(jnp.int32).reshape(1)
    lists = sort(*flat, counts, mine)
    moved = [
        lax.ppermute(lists[d], "samp", [(i, (i + d) % 4) for i in range(4)]) for d in (2, 1, 3)
    ]
    consts = tables(lists[0], kernel.T)
    sent = spectra(moved, *consts)
    received = lax.all_to_all(sent.reshape(128, 1, TILES * 128), ("band", "samp"), 0, 0, tiled=True)
    wigner = wigner.reshape(PER_DEV, WROWS, RT)
    head, d = early(wigner)
    sky = sky_of(received.reshape(128 * TILES, 128), wigner, head, beam.T, d)
    return jnp.transpose(sky, (1, 0, 2))


def solution(mesh):
    split_both = P("band", "samp")
    placed = (split_both,) * 6 + (P(), P("band", "samp", None, None, None), P())
    return jax.shard_map(
        body, mesh=mesh, in_specs=placed, out_specs=P("band", "samp", None), check_vma=False
    )
```

```python
import jax
import jax.numpy as jnp
import numpy as np
from jax import lax
from jax.experimental import pallas as pl
from jax.experimental.pallas import tpu as pltpu
from jax.sharding import PartitionSpec as P


PHI = 8192
K = 33
LB = 64
RT = 128
PER_DEV = 20
ROWS = 32
CELL_ROWS = 560
TILES = 11
HEAD = 2
KSTEP = 11
WROWS = K * LB
WPAD = WROWS
BF = jnp.bfloat16


def split_host(x):
    x = np.asarray(x, np.float32)
    hi = x.astype(BF)
    lo = (x - hi.astype(np.float32)).astype(BF)
    return np.stack([hi, lo])


def host_tables():
    a = np.arange(16)
    cl = np.arange(16)
    ang = 2 * np.pi * ((a[:, None] * cl[None, :]) % 16) / 16
    fc, fs = np.cos(ang), -np.sin(ang)
    even = np.stack([fc[:8, n] for n in (0, 4, 2, 6, 8)] + [fs[:8, n] for n in (4, 2, 6)], 1)
    odd = np.stack([f[:8, n] for f in (fc, fs) for n in (5, 1, 7, 3)], 1)
    f_main = np.stack([np.tile(np.repeat(x, 32, 1), (2, 1)) for x in (even, odd)])
    f_last = np.zeros((128, 256))
    f_last[:16, :16] = fc
    f_last[:16, 128:144] = fs
    b = np.arange(256)
    e, i = np.arange(5)[:, None], np.arange(16)[None, :]
    halves = []
    for odd in range(2):
        m2 = (5 * (2 * i + (e + odd) % 2) + e).reshape(-1)
        ang = 2 * np.pi * ((m2[:, None] * b[None, :]) % 512) / 512
        halves.append(np.concatenate([np.cos(ang), np.sin(ang)], 0))
    w_phi = np.stack(halves)
    lanes = np.concatenate([np.arange(512) // 32, np.where(np.arange(128) < 16, np.arange(128), 0)])
    ang = 2 * np.pi * (16 * np.arange(33)[:, None] * lanes[None, :]) / PHI
    t_hi = np.stack([np.cos(ang), np.sin(ang)]).astype(np.float32)
    ang = 2 * np.pi * (np.arange(16)[:, None] * lanes[None, :]) / PHI
    t_lo = np.stack([np.cos(ang), np.sin(ang)]).astype(np.float32)
    k = np.arange(K)
    ang = 2 * np.pi * ((k[:, None] * k[None, :]) % K) / K
    d = np.zeros((80, 80))
    c, s = np.cos(ang), np.sin(ang)
    d[0:66:2, 0:32], d[0:66:2, 64] = c[:, :32], c[:, 32]
    d[0:66:2, 32:64], d[0:66:2, 65] = s[:, :32], s[:, 32]
    d[1:66:2, 0:32], d[1:66:2, 64] = -s[:, :32], -s[:, 32]
    d[1:66:2, 32:64], d[1:66:2, 65] = c[:, :32], c[:, 32]
    return split_host(f_main), split_host(f_last), split_host(w_phi), t_hi, t_lo, split_host(d)


F_MAIN, F_LAST, W_PHI, TW_HI, TW_LO, D_PSI = host_tables()


def split(x):
    hi = x.astype(BF)
    lo = (x - hi.astype(jnp.float32)).astype(BF)
    return hi, lo


def dot(x, y):
    return jnp.dot(x, y, preferred_element_type=jnp.float32)


def dot_nt(x, y):
    return lax.dot_general(x, y, (((1,), (1,)), ((), ())), preferred_element_type=jnp.float32)


def sort_kernel(
    tod_h, cyc_h, phi_h, psi_h, off_h, cnt_ref, mine_ref, out0, out1, out2, out3,
    tod_ref, int_ref, data_ref, to_ref, o_ref, first_ref, first_s, buf_ref, sems,
):
    copies = [pltpu.make_async_copy(tod_h, tod_ref, sems.at[0])]
    for i, src in enumerate((cyc_h, phi_h, psi_h, off_h)):
        copies.append(pltpu.make_async_copy(src, int_ref.at[i], sems.at[1 + i]))
    for c in copies:
        c.start()
    for c in copies:
        c.wait()
    slot = lax.broadcasted_iota(jnp.int32, (ROWS, 128), 0) * 128 + lax.broadcasted_iota(
        jnp.int32, (ROWS, 128), 1
    )
    cyc = jnp.where(slot < cnt_ref[0, 0], (int_ref[0] - mine_ref[0]) & 3, 4)

    def below(n):
        return (
            lax.broadcasted_iota(jnp.int32, (n, n), 0) < lax.broadcasted_iota(jnp.int32, (n, n), 1)
        ).astype(jnp.float32).astype(BF)

    earlier = below(128)
    rows_before = (
        lax.broadcasted_iota(jnp.int32, (ROWS, ROWS), 1) < lax.broadcasted_iota(jnp.int32, (ROWS, ROWS), 0)
    ).astype(jnp.float32).astype(BF)
    every = jnp.ones((128, 128), BF)
    lane0 = lax.broadcasted_iota(jnp.int32, (ROWS, 128), 1)
    row0 = lax.broadcasted_iota(jnp.int32, (ROWS, 128), 0)
    place = jnp.full((ROWS, 128), -1.0, jnp.float32)
    ahead = jnp.zeros((ROWS, 128), jnp.float32)
    starts, shifts = [], []

    def on_lanes(x, shift):
        return jnp.sum(jnp.where(lane0 == row0 + shift, x, 0.0), axis=0, keepdims=True)

    for c in range(4):
        m = (cyc == c).astype(jnp.float32).astype(BF)
        total = dot(m, every)
        start = dot(rows_before, total.astype(BF))
        starts.append(on_lanes(start + total, 1))
        shifts.append(on_lanes(start - ahead, 0))
        place = jnp.where(cyc == c, ahead + dot(m, earlier), place)
        ahead = ahead + total
    first_ref[...] = jnp.concatenate(starts + shifts, 0).astype(jnp.int32)
    to_smem = pltpu.make_async_copy(first_ref, first_s, sems.at[5])
    to_smem.start()
    place = place.astype(jnp.int32)
    to_ref[0] = (place >> 4).astype(jnp.float32)
    to_ref[1] = (place & 15).astype(jnp.float32)

    def channel(i, x):
        data_ref[pl.ds(i, ROWS, stride=8), :] = x

    tod = tod_ref[...]
    hi = tod.astype(BF).astype(jnp.float32)
    mid = (tod - hi).astype(BF).astype(jnp.float32)
    channel(0, hi)
    channel(1, mid)
    channel(2, tod - hi - mid)
    channel(3, (int_ref[1] >> 7).astype(jnp.float32))
    channel(4, (int_ref[1] & 127).astype(jnp.float32))
    channel(5, int_ref[2].astype(jnp.float32))
    channel(6, int_ref[3].astype(jnp.float32))
    channel(7, jnp.zeros((ROWS, 128), jnp.float32))

    sub = lax.broadcasted_iota(jnp.int32, (16, 128), 0).astype(jnp.float32).astype(BF)
    zero = jnp.zeros((16, 128), BF)
    one = jnp.ones((16, 128), BF)

    def route(i, carry):
        hi = jnp.broadcast_to(to_ref[0, pl.ds(i, 1), :], (16, 128)).astype(BF)
        lo = jnp.broadcast_to(to_ref[1, pl.ds(i, 1), :], (16, 128)).astype(BF)
        ones = jnp.where(lo == sub, one, zero)
        chosen = jnp.concatenate([jnp.where(hi == float(h), ones, zero) for h in range(8)], 0)
        row = data_ref[pl.ds(pl.multiple_of(i * 8, 8), 8), :].astype(BF)
        o_ref[pl.ds(pl.multiple_of(i * 8, 8), 8), :] = dot_nt(row, chosen)
        return carry

    lax.fori_loop(0, ROWS, route, 0, unroll=ROWS)
    to_smem.wait()
    lane = lax.broadcasted_iota(jnp.int32, (8, 128), 1)

    def append(i, held):
        out = []
        moved = o_ref[pl.ds(pl.multiple_of(i * 8, 8), 8), :]
        for c in range(4):
            begin = first_s[c, i]
            after = first_s[c, i + 1]
            row = begin >> 7
            here = begin & 127
            end = here + after - begin
            own = pltpu.roll(moved, first_s[4 + c, i] & 127, 1)
            full = held[c] + jnp.where((lane >= here) & (lane < end), own, 0.0)
            over = jnp.where(lane < end - 128, own, 0.0)
            at = pl.multiple_of((c * 34 + row) * 8, 8)
            buf_ref[pl.ds(at, 8), :] = full
            buf_ref[pl.ds(at + 8, 8), :] = over
            out.append(jnp.where((after >> 7) > row, over, full))
        return tuple(out)

    lax.fori_loop(0, ROWS, append, (jnp.zeros((8, 128), jnp.float32),) * 4, unroll=ROWS)
    for c, out_ref in enumerate((out0, out1, out2, out3)):
        valid = slot < first_s[c, ROWS]

        def take(ch):
            return buf_ref[pl.ds(c * 34 * 8 + ch, ROWS, stride=8), :]

        out_ref[0] = jnp.where(valid, take(0) + take(1) + take(2), 0.0)
        out_ref[1] = jnp.where(valid, take(3) * 128.0 + take(4), 0.0)
        out_ref[2] = jnp.where(valid, take(5), -1.0)
        out_ref[3] = jnp.where(valid, take(6), 0.0)


def prepare(lists, kb_ref, s_ref):
    spare = len(lists) * ROWS
    ends, skips = [], []
    total = jnp.int32(0)
    s_ref[0, spare : spare + 8, :] = jnp.full((8, 128), -1.0, jnp.float32)
    for ch in range(1, 8):
        s_ref[ch, spare : spare + 8, :] = jnp.zeros((8, 128), jnp.float32)
    for s, g_ref in enumerate(lists):
        tod = g_ref[0]
        phi = g_ref[1].astype(jnp.int32)
        psi = g_ref[2].astype(jnp.int32)
        off = g_ref[3].astype(jnp.int32)
        live = psi >= 0
        count = jnp.sum(live.astype(jnp.float32)).astype(jnp.int32)
        rows = (count + 127) >> 7
        total = total + rows
        ends.append(total)
        skips.append(ROWS - rows)
        first = jnp.where(phi == 0, PHI - 1, phi - 1)
        b_hi = (first & 511) >> 4
        is_last = psi == 32
        at = pl.ds(s * ROWS, ROWS)
        a_hi, a_lo = first >> 12, (first >> 9) & 7
        column = jnp.where(is_last, b_hi * 16 + (first >> 9), a_hi * 256 + psi * 8 + a_lo)
        s_ref[0, at, :] = jnp.where(live, column >> 4, -1).astype(jnp.float32)
        s_ref[1, at, :] = (column & 15).astype(jnp.float32)
        s_ref[2, at, :] = jnp.where(is_last, 33, b_hi).astype(jnp.float32)
        s_ref[3, at, :] = (first & 15).astype(jnp.float32)
        for t in range(4):
            weight = jnp.zeros((ROWS, 128), jnp.float32)
            for o in range(8):
                entry = jnp.concatenate([kb_ref[t * 8 + o]] * (ROWS // 8), 0)
                weight = jnp.where(off == o, entry, weight)
            s_ref[4 + t, at, :] = (tod * weight).astype(BF).astype(jnp.float32)
    return ends, skips, total


def deposit(block, s_ref, acc_ref, ends, skips, total):
    spare = len(ends) * ROWS
    sub = lax.broadcasted_iota(jnp.int32, (16, 128), 0).astype(jnp.float32).astype(BF)
    zero = jnp.zeros((16, 128), BF)
    one = jnp.ones((16, 128), BF)

    def build(first):
        left, right = [], []
        for j in range(block):
            f = first + j
            r = f
            for s in range(len(ends)):
                r = r + jnp.where(f >= ends[s], skips[s], 0)
            r = jnp.minimum(r, spare)

            def row(ch):
                v = s_ref[ch, pl.ds(r, 1), :]
                return jnp.broadcast_to(v, (16, 128)).astype(BF)

            n_hi, n_lo, m_hi, m_lo = row(0), row(1), row(2), row(3)
            a0, a1, a2, a3 = row(4), row(5), row(6), row(7)
            ones = jnp.where(n_lo == sub, one, zero)
            d = sub - m_lo
            main = jnp.where(
                d == 0.0, a0, jnp.where(d == 1.0, a1, jnp.where(d == 2.0, a2, jnp.where(d == 3.0, a3, zero)))
            )
            spill = jnp.where(
                d == -15.0, a1, jnp.where(d == -14.0, a2, jnp.where(d == -13.0, a3, zero))
            )
            left.append(jnp.concatenate([jnp.where(n_hi == float(h), ones, zero) for h in range(32)], 0))
            here = [m_hi == float(h) for h in range(35)]
            right.append(
                jnp.concatenate(
                    [jnp.where(here[0], main, zero)]
                    + [
                        jnp.where(here[h], main, jnp.where(here[h - 1], spill, zero))
                        for h in range(1, 35)
                    ],
                    0,
                )
            )
        return left, right

    def step(i, carry):
        left, right = build(i * block)
        sums = None
        for j in range(0, block, 2):
            part = dot_nt(
                jnp.concatenate(right[j : j + 2], 1), jnp.concatenate(left[j : j + 2], 1)
            )
            sums = part if sums is None else sums + part
        acc_ref[...] += sums
        return carry

    lax.fori_loop(0, (total + block - 1) // block, step, 0)


def tables_kernel(
    g_ref, fm_h, fl_h, th_h, tl_h, kern_h, s1_ref, fl_ref, th_ref, tl_ref, kb_ref, acc_ref,
    fm_ref, kern_ref, s_ref, sems,
):
    pairs = (
        (fm_h, fm_ref), (fl_h, fl_ref), (th_h, th_ref), (tl_h, tl_ref), (kern_h, kern_ref)
    )
    copies = [pltpu.make_async_copy(a, b, sems.at[i]) for i, (a, b) in enumerate(pairs)]
    for c in copies:
        c.start()
    copies[4].wait()
    for t in range(4):
        for o in range(8):
            kb_ref[t * 8 + o] = jnp.full((8, 128), kern_ref[t, o], jnp.float32)
    acc_ref[...] = jnp.zeros_like(acc_ref)
    deposit(8, s_ref, acc_ref, *prepare((g_ref,), kb_ref, s_ref))
    copies[0].wait()
    ahead = (lax.broadcasted_iota(jnp.int32, (16, 256), 1) & 31) - (
        lax.broadcasted_iota(jnp.int32, (16, 256), 0) >> 3
    )
    ahead = ahead.astype(jnp.float32).astype(BF)
    for q in range(0, 32, 2):
        keep = ahead == float(q)
        for part in range(2):
            for odd in range(2):
                s1_ref[part, odd, q * 8 : q * 8 + 16, :] = jnp.where(
                    keep, fm_ref[part, odd], jnp.zeros((16, 256), BF)
                )
    for c in copies[1:4]:
        c.wait()


def spectra_kernel(
    g1, g2, g3, s1_ref, fl_ref, th_ref, tl_ref, kb_ref, own_ref, w_h, out_ref,
    s_ref, acc_ref, last_ref, zh_ref, zl_ref, w_ref, w_sem,
):
    w_copy = pltpu.make_async_copy(w_h, w_ref, w_sem.at[0])
    w_copy.start()
    acc_ref[...] = own_ref[...]
    deposit(12, s_ref, acc_ref, *prepare((g1, g2, g3), kb_ref, s_ref))

    def chunk(r0, at):
        tile = acc_ref[r0 : r0 + 16, (at // 8) * 128 : (at // 8) * 128 + 128]
        shift = (at % 8) * 16
        return tile if shift == 0 else pltpu.roll(tile, 128 - shift, 1)

    for h in range(33):
        tile = jnp.zeros((16, 128), jnp.float32)
        if h < 32:
            tile = tile + chunk(528, h)
        if h > 0:
            tile = tile + chunk(544, h - 1)
        last_ref[h * 16 : (h + 1) * 16, :] = tile

    quarter = lax.broadcasted_iota(jnp.int32, (16, 128), 1) >> 5
    none = jnp.zeros((16, 128), jnp.float32)

    def merge(even, odd):
        here = jnp.where(quarter & 1 == 0, even, odd)
        there = jnp.where(quarter & 1 == 0, pltpu.roll(even, 96, 1), pltpu.roll(odd, 32, 1))
        return here, there

    def pick(at0, at2, odd):
        return jnp.where(quarter == 0, at0, jnp.where(quarter == 2, at2, odd))

    def first_stage(r0, rows):
        at = pl.ds(r0, rows)
        low, high = acc_ref[at, :256], acc_ref[at, 256:]
        y = []
        for odd, x in enumerate((low + high, low - high)):
            xh, xl = split(x)
            y.append(dot(xh, s1_ref[0, odd]) + dot(xl, s1_ref[0, odd]) + dot(xh, s1_ref[1, odd]))
        xh, xl = split(last_ref[at, :])
        y_last = dot(xh, fl_ref[0]) + dot(xl, fl_ref[0]) + dot(xh, fl_ref[1])
        out = []
        for i in range(rows // 16):
            h = r0 // 16 + i
            ch, sh = th_ref[0, h : h + 1, :], th_ref[1, h : h + 1, :]
            cw = ch * tl_ref[0] - sh * tl_ref[1]
            sw = sh * tl_ref[0] + ch * tl_ref[1]
            at = slice(i * 16, (i + 1) * 16)
            a0, a1, b0, b1 = (
                v
                for g in range(2)
                for v in merge(*(x[at, g * 128 : (g + 1) * 128] for x in y))
            )
            ra0, ra1, rb0, rb1 = (pltpu.roll(v, 64, 1) for v in (a0, a1, b0, b1))
            yr = jnp.concatenate(
                [a0, a1, pick(b0, a1, ra1), pick(a1, a0, ra0), y_last[at, :128]], 1
            )
            yi = jnp.concatenate(
                [pick(none, b0, b0), b1, -pick(none, b1, rb1), -pick(b1, b0, rb0), y_last[at, 128:]], 1
            )
            out.append((yr * cw + yi * sw, yi * cw - yr * sw))
        return out

    halo = first_stage(512, 16)[0]
    for r0 in range(0, 256, 128):
        for i, (near, far) in enumerate(zip(first_stage(r0, 128), first_stage(r0 + 256, 128))):
            if r0 == 0 and i == 0:
                near = (near[0] + halo[0], near[1] + halo[1])
            at = slice(r0 + i * 16, r0 + (i + 1) * 16)
            for odd in range(2):
                zr, zi = (n - f if odd else n + f for n, f in zip(near, far))
                rh, rl = split(zr)
                ih, il = split(zi)
                for g in range(5):
                    take = slice(g * 128, (g + 1) * 128)
                    re, im = slice(g * 256, g * 256 + 128), slice(g * 256 + 128, g * 256 + 256)
                    zh_ref[odd, at, re] = rh[:, take]
                    zh_ref[odd, at, im] = ih[:, take]
                    zl_ref[odd, at, re] = rl[:, take]
                    zl_ref[odd, at, im] = il[:, take]

    w_copy.wait()

    def put(s_to, tile_no, half, value):
        first = (4 * half + s_to) * TILES + tile_no
        out_ref[pl.ds(first, 16, stride=8 * TILES), :] = value

    lanes = lax.broadcasted_iota(jnp.int32, (16, 128), 1)
    last_parts = [[[None] * 5 for _ in range(2)] for _ in range(2)]
    for g in range(5):
        take = slice(g * 256, (g + 1) * 256)
        for odd in range(2):
            zh, zl = zh_ref[odd, :, take], zl_ref[odd, :, take]
            p = dot(w_ref[0, odd], zh) + dot(w_ref[1, odd], zh) + dot(w_ref[0, odd], zl)
            parts = (p[:80, :128] + p[80:, 128:], p[:80, 128:] - p[80:, :128])
            if g < 4:
                for c in range(2):
                    for e in range(5):
                        s_to, t = divmod(e * 4 + g, 5)
                        put(s_to, c * 5 + t, (e + odd) % 2, parts[c][e * 16 : (e + 1) * 16])
                continue
            for c in range(2):
                for e in range(5):
                    last_parts[odd][c][e] = parts[c][e * 16 : (e + 1) * 16]
    for s_to in range(4):
        for half in range(2):
            row = jnp.zeros((16, 128), jnp.float32)
            for c in range(2):
                j = 0
                while j < PER_DEV:
                    e, cl = divmod(PER_DEV * s_to + j, 16)
                    length = min(16 - cl, PER_DEV - j)
                    to = 64 * c + j
                    piece = last_parts[(e + half) % 2][c][e]
                    shift = (to - cl) % 128
                    piece = piece if shift == 0 else pltpu.roll(piece, shift, 1)
                    row = jnp.where((lanes >= to) & (lanes < to + length), piece, row)
                    j += length
            put(s_to, 10, half, row)


def early_kernel(wig_h, d_h, head_ref, d_ref, sems):
    copies = [pltpu.make_async_copy(d_h, d_ref, sems.at[HEAD])]
    for m in range(HEAD):
        copies.append(
            pltpu.make_async_copy(wig_h.at[m], head_ref.at[m, pl.ds(0, WROWS)], sems.at[m])
        )
    for c in copies:
        c.start()
    for c in copies:
        c.wait()


def sky_kernel(
    r_ref, wig_h, head_ref, beam_ref, d_ref, out_h, wbuf, bb_ref, gh_ref, gl_ref, h_ref, out_ref, sems, out_sem
):
    def fetch(m):
        return pltpu.make_async_copy(
            wig_h.at[m], wbuf.at[m - HEAD, pl.ds(0, WROWS)], sems.at[m - HEAD]
        )

    for m in range(HEAD, PER_DEV):
        fetch(m).start()

    beam = beam_ref[...].T
    for k in range(K):
        bb_ref[k * LB : (k + 1) * LB, :] = jnp.broadcast_to(beam[:, k : k + 1], (LB, 128))

    def tile(t):
        return r_ref[pl.ds(t, 128, stride=TILES), :].T

    rem = tile(10)
    sub = lax.broadcasted_iota(jnp.int32, (16, 128), 0)
    for t in range(5):
        planes = (tile(t), tile(5 + t))
        for jj in range(4):
            j = t * 4 + jj
            half = slice((j % 2) * 128, (j % 2) * 128 + 128)
            for c in range(2):
                hi, lo = split(planes[c][jj * 32 : (jj + 1) * 32])
                gh_ref[j // 2, c * 32 : (c + 1) * 32, half] = hi
                gl_ref[j // 2, c * 32 : (c + 1) * 32, half] = lo
            extra = jnp.where(sub == 0, rem[j : j + 1], jnp.where(sub == 1, rem[64 + j : 65 + j], 0.0))
            hi, lo = split(extra)
            gh_ref[j // 2, 64:80, half] = hi
            gl_ref[j // 2, 64:80, half] = lo
    for i in range(PER_DEV // 2):
        h = dot(d_ref[0], gh_ref[i]) + dot(d_ref[1], gh_ref[i]) + dot(d_ref[0], gl_ref[i])
        h_ref[2 * i] = h[:, :128]
        h_ref[2 * i + 1] = h[:, 128:]

    ones = jnp.ones((16, 128), BF)

    def orders(m, w_ref, at_m):
        def some(kk, sums):
            sums = [list(x) for x in sums]
            for j in range(KSTEP):
                k = kk * KSTEP + j
                base = pl.multiple_of(k * LB, LB)
                h = [
                    [
                        jnp.broadcast_to(h_ref[m + n, pl.ds(2 * k + c, 1), :], (8, 128))
                        for c in range(2)
                    ]
                    for n in range(2)
                ]
                for i in range(8):
                    b = bb_ref[pl.ds(base + i * 8, 8), :]
                    for n in range(2):
                        w = w_ref[at_m + n, pl.ds(base + i * 8, 8), :] * b
                        sums[n][i] = sums[n][i] + w * h[n][0]
                        sums[n][8 + i] = sums[n][8 + i] + w * h[n][1]
            return tuple(tuple(x) for x in sums)

        sums = ((jnp.zeros((8, 128), jnp.float32),) * 16,) * 2
        sums = lax.fori_loop(0, K // KSTEP, some, sums)
        for n in range(2):
            both = jnp.concatenate(sums[n], 0)
            hi, lo = split(both)
            tail = (both - hi.astype(jnp.float32) - lo.astype(jnp.float32)).astype(BF)
            res = dot_nt(ones, hi) + dot_nt(ones, lo) + dot_nt(ones, tail)
            out_ref[m + n] = res[0:1]

    for m in range(0, HEAD, 2):
        orders(m, head_ref, m)

    def streamed(i, carry):
        m = HEAD + 2 * i
        fetch(m).wait()
        fetch(m + 1).wait()
        orders(m, wbuf, 2 * i)
        return carry

    lax.fori_loop(0, (PER_DEV - HEAD) // 2, streamed, 0)
    out_copy = pltpu.make_async_copy(out_ref, out_h, out_sem.at[0])
    out_copy.start()
    out_copy.wait()


def vmem():
    return pl.BlockSpec(memory_space=pltpu.VMEM)


def hbm():
    return pl.BlockSpec(memory_space=pltpu.HBM)


def stay(*arrays):
    return [pltpu.with_memory_space_constraint(jnp.asarray(x), pltpu.HBM) for x in arrays]


def sort(tod, cycle, phi_cell, psi_bin, offset, counts, mine):
    return pl.pallas_call(
        sort_kernel,
        out_shape=[jax.ShapeDtypeStruct((4, ROWS, 128), jnp.float32)] * 4,
        in_specs=[hbm()] * 5 + [pl.BlockSpec(memory_space=pltpu.SMEM)] * 2,
        out_specs=[vmem()] * 4,
        scratch_shapes=[
            pltpu.VMEM((ROWS, 128), jnp.float32),
            pltpu.VMEM((4, ROWS, 128), jnp.int32),
            pltpu.VMEM((ROWS * 8, 128), jnp.float32),
            pltpu.VMEM((2, ROWS, 128), jnp.float32),
            pltpu.VMEM((ROWS * 8, 128), jnp.float32),
            pltpu.VMEM((8, 128), jnp.int32),
            pltpu.SMEM((8, 128), jnp.int32),
            pltpu.VMEM((4 * 34 * 8, 128), jnp.float32),
            pltpu.SemaphoreType.DMA((6,)),
        ],
        compiler_params=pltpu.CompilerParams(vmem_limit_bytes=8 << 20),
        name="sort",
    )(*stay(tod, cycle, phi_cell, psi_bin, offset), counts, mine)


def tables(own, kernel):
    shapes = ((2, 2, 256, 256), F_LAST.shape, TW_HI.shape, TW_LO.shape, (32, 8, 128), (CELL_ROWS, 512))
    types = (BF, BF) + (jnp.float32,) * 4
    return pl.pallas_call(
        tables_kernel,
        out_shape=[pltpu.VMEM(s, t) for s, t in zip(shapes, types)],
        in_specs=[vmem()] + [hbm()] * 5,
        out_specs=[vmem()] * 6,
        scratch_shapes=[
            pltpu.VMEM(F_MAIN.shape, BF),
            pltpu.SMEM((4, 8), jnp.float32),
            pltpu.VMEM((8, ROWS + 8, 128), jnp.float32),
            pltpu.SemaphoreType.DMA((5,)),
        ],
        compiler_params=pltpu.CompilerParams(vmem_limit_bytes=16 << 20),
        name="tables",
    )(own, *stay(F_MAIN, F_LAST, TW_HI, TW_LO, kernel))


def spectra(lists, *consts):
    return pl.pallas_call(
        spectra_kernel,
        out_shape=jax.ShapeDtypeStruct((128 * TILES, 128), jnp.float32),
        in_specs=[vmem()] * 9 + [hbm()],
        out_specs=vmem(),
        scratch_shapes=[
            pltpu.VMEM((8, 3 * ROWS + 8, 128), jnp.float32),
            pltpu.VMEM((CELL_ROWS, 512), jnp.float32),
            pltpu.VMEM((528, 128), jnp.float32),
            pltpu.VMEM((2, 256, 1280), BF),
            pltpu.VMEM((2, 256, 1280), BF),
            pltpu.VMEM(W_PHI.shape, BF),
            pltpu.SemaphoreType.DMA((1,)),
        ],
        compiler_params=pltpu.CompilerParams(vmem_limit_bytes=20 << 20),
        name="spectra",
    )(*lists, *consts, *stay(W_PHI))


def early(wigner):
    return pl.pallas_call(
        early_kernel,
        out_shape=[pltpu.VMEM((HEAD, WPAD, RT), jnp.float32), pltpu.VMEM(D_PSI.shape, BF)],
        in_specs=[hbm()] * 2,
        out_specs=[vmem()] * 2,
        scratch_shapes=[pltpu.SemaphoreType.DMA((HEAD + 1,))],
        compiler_params=pltpu.CompilerParams(vmem_limit_bytes=4 << 20),
        name="early",
    )(*stay(wigner, D_PSI))


def sky_of(received, wigner, head, beam, d):
    return pl.pallas_call(
        sky_kernel,
        out_shape=pltpu.HBM((PER_DEV, 1, 2 * LB), jnp.float32),
        in_specs=[vmem(), hbm(), vmem(), vmem(), vmem()],
        out_specs=hbm(),
        scratch_shapes=[
            pltpu.VMEM((PER_DEV - HEAD, WPAD, RT), jnp.float32),
            pltpu.VMEM((WROWS, 128), jnp.float32),
            pltpu.VMEM((PER_DEV // 2, 80, 256), BF),
            pltpu.VMEM((PER_DEV // 2, 80, 256), BF),
            pltpu.VMEM((PER_DEV, 80, 128), jnp.float32),
            pltpu.VMEM((PER_DEV, 1, 2 * LB), jnp.float32),
            pltpu.SemaphoreType.DMA((PER_DEV - HEAD,)),
            pltpu.SemaphoreType.DMA((1,)),
        ],
        compiler_params=pltpu.CompilerParams(vmem_limit_bytes=36 << 20),
        name="sky",
    )(received, *stay(wigner), head, beam, d)


def body(tod, cycle, phi_cell, psi_bin, offset, counts, kernel, wigner, beam):
    flat = [x.reshape(ROWS, 128) for x in (tod, cycle, phi_cell, psi_bin, offset)]
    mine = lax.axis_index("samp").astype(jnp.int32).reshape(1)
    lists = sort(*flat, counts, mine)
    moved = [
        lax.ppermute(lists[d], "samp", [(i, (i + d) % 4) for i in range(4)]) for d in (2, 1, 3)
    ]
    consts = tables(lists[0], kernel.T)
    sent = spectra(moved, *consts)
    received = lax.all_to_all(sent.reshape(128, 1, TILES * 128), ("band", "samp"), 0, 0, tiled=True)
    wigner = wigner.reshape(PER_DEV, WROWS, RT)
    head, d = early(wigner)
    sky = sky_of(received.reshape(128 * TILES, 128), wigner, head, beam.T, d)
    return jnp.transpose(sky, (1, 0, 2))


def solution(mesh):
    split_both = P("band", "samp")
    placed = (split_both,) * 6 + (P(), P("band", "samp", None, None, None), P())
    return jax.shard_map(
        body, mesh=mesh, in_specs=placed, out_specs=P("band", "samp", None), check_vma=False
    )
```
